16 devices in a mesh: sys: 2 (over y, z), row: 8 (over x, core).
Axes of the slice: x: 4, y: 2, z: 1, core: 2. Of those that a mesh axis runs over, the one named last changes fastest.
The devices are a block of a 4x4x8 slice.
Arguments:
- positions: bfloat16 [32768, 384], P(('sys', 'row')), parts along dimension 0
- charges: float32 [32768], P(('sys', 'row')), parts along dimension 0
- counts: int32 [16], P(('sys', 'row')), parts along dimension 0
Outputs:
- output 1: float32 [32768, 384], P(('sys', 'row')), parts along dimension 0
- output 2: float32 [2], P('sys'), parts along dimension 0
There are 2 independent parts. The reference program is written for one: setup_inputs(seed, part) draws one part's arguments, and reference() takes and returns one part's arrays. A program takes and returns all parts, laid end to end along the dimension named above; each array names one.
All inputs are finite; a program needn't handle non-finite values.
Results may differ from the reference program's by a relative error of at most 0.001.
Values are sent between devices in bfloat16 or wider.
A program may use at most 768 MiB of HBM per device.

```python
import jax
import jax.numpy as jnp
from jax import lax

BLOCK_ROWS = 2048
D = 384
RING_SIZE = 8
NUM_ROWS = RING_SIZE * BLOCK_ROWS
ROW_TILE = min(BLOCK_ROWS, 256)


def setup_inputs(seed: int = 0, part: int = 0) -> dict:
    part_key = jax.random.fold_in(jax.random.key(seed), part)
    sub_keys = jax.random.split(part_key, 6)
    positions = jax.random.normal(sub_keys[0], (NUM_ROWS, D), jnp.float32).astype(jnp.bfloat16)
    sign_vals = jnp.where(jax.random.bernoulli(sub_keys[1], 0.5, (NUM_ROWS,)), 1.0, -1.0)
    magnitude = jax.random.uniform(sub_keys[2], (NUM_ROWS,), jnp.float32, 0.5, 1.5)
    charges = (sign_vals * magnitude).astype(jnp.float32)
    counts = jax.random.randint(sub_keys[3], (RING_SIZE,), BLOCK_ROWS // 16, BLOCK_ROWS + 1)
    full_slot = jax.random.randint(sub_keys[4], (), 0, RING_SIZE)
    small_slot = (full_slot + jax.random.randint(sub_keys[5], (), 1, RING_SIZE)) % RING_SIZE
    counts = counts.at[full_slot].set(BLOCK_ROWS).at[small_slot].set(BLOCK_ROWS // 16)
    return {'positions': positions, 'charges': charges, 'counts': counts.astype(jnp.int32)}


def reference(positions, charges, counts):
    is_valid = jnp.arange(BLOCK_ROWS)[None, :] < counts[:, None]
    live_q = jnp.where(is_valid, charges.reshape(RING_SIZE, BLOCK_ROWS), 0.0).reshape(NUM_ROWS)
    pos_f32 = positions.astype(jnp.float32)
    sq_norm = jnp.sum(pos_f32 * pos_f32, axis=1)
    col_ids = jnp.arange(NUM_ROWS)
    neg_scale = -0.5 / D
    inv_len2 = 1.0 / D

    def tile_terms(tile_idx):
        row_start = tile_idx * ROW_TILE
        row_block = lax.dynamic_slice(positions, (row_start, 0), (ROW_TILE, D))
        row_q = lax.dynamic_slice(live_q, (row_start,), (ROW_TILE,))
        row_sq = lax.dynamic_slice(sq_norm, (row_start,), (ROW_TILE,))
        gram_mat = jnp.dot(row_block, positions.T, preferred_element_type=jnp.float32)
        dist_sq = jnp.maximum(row_sq[:, None] + sq_norm[None, :] - 2.0 * gram_mat, 0.0)
        weight = row_q[:, None] * live_q[None, :] * jnp.exp(dist_sq * neg_scale)
        row_ids = row_start + jnp.arange(ROW_TILE)
        weight = jnp.where(row_ids[:, None] == col_ids[None, :], 0.0, weight)
        pulled = jnp.dot(weight.astype(jnp.bfloat16), positions, preferred_element_type=jnp.float32)
        row_force = (jnp.sum(weight, axis=1)[:, None] * row_block.astype(jnp.float32) - pulled) * inv_len2
        return row_force, jnp.sum(weight)

    tile_forces, tile_energy = lax.map(tile_terms, jnp.arange(NUM_ROWS // ROW_TILE))
    return tile_forces.reshape(NUM_ROWS, D), (0.5 * jnp.sum(tile_energy)).reshape(1)
```

```python
import functools
import math

import jax
import jax.numpy as jnp
from jax import lax
from jax.experimental import pallas as pl
from jax.experimental.pallas import tpu as pltpu
from jax.sharding import PartitionSpec as P


LANES = 128
TILE_I = 256
TILE_J = 512
MESH = pl.DeviceIdType.MESH
VMEM_SPEC = pl.BlockSpec(memory_space=pltpu.VMEM)
SMEM_SPEC = pl.BlockSpec(memory_space=pltpu.SMEM)


def exchange_kernel(n, src_ref, out_ref, send_sem, recv_sem, local_sem):
    me = lax.axis_index('row')
    barrier = pltpu.get_barrier_semaphore()
    for off in range(1, n):
        pl.semaphore_signal(barrier, inc=1, device_id={'row': lax.rem(me + off, n)}, device_id_type=MESH)
    own = pltpu.make_async_copy(src_ref, out_ref.at[me], local_sem)
    own.start()
    pl.semaphore_wait(barrier, n - 1)
    copies = []
    for off in range(1, n):
        copies.append(pltpu.make_async_remote_copy(
            src_ref=src_ref, dst_ref=out_ref.at[me], send_sem=send_sem.at[off - 1], recv_sem=recv_sem.at[off - 1],
            device_id={'row': lax.rem(me + off, n)}, device_id_type=MESH))
    for copy in copies:
        copy.start()
    own.wait()
    for copy in copies:
        copy.wait()


def exchange(src, n, collective_id):
    return pl.pallas_call(
        functools.partial(exchange_kernel, n),
        out_shape=jax.ShapeDtypeStruct((n,) + src.shape, src.dtype),
        in_specs=[pl.BlockSpec(memory_space=pl.ANY)],
        out_specs=pl.BlockSpec(memory_space=pl.ANY),
        scratch_shapes=[pltpu.SemaphoreType.DMA((n - 1,)), pltpu.SemaphoreType.DMA((n - 1,)), pltpu.SemaphoreType.DMA],
        compiler_params=pltpu.CompilerParams(collective_id=collective_id, has_side_effects=True),
        cost_estimate=pl.CostEstimate(flops=0, bytes_accessed=8 << 20, transcendentals=0),
        name=f'exchange_{collective_id}',
    )(src)


def pair_tiles(row_count, col_count, x_i, h_i, c_i, x_j, col_at, cols, scale, t_ref, s_ref, diag):
    n_i = pl.cdiv(row_count, TILE_I)
    n_j = pl.cdiv(col_count, TILE_J)

    def row_step(i, carry):
        rows = pl.ds(pl.multiple_of(i * TILE_I, TILE_I), TILE_I)

        def col_step(j, carry):
            j0 = pl.multiple_of(j * TILE_J, TILE_J)
            x_col = x_j[pl.ds(j0, TILE_J), :]
            gram = lax.dot_general(x_i[rows, :], x_col, (((1,), (1,)), ((), ())), preferred_element_type=jnp.float32)
            h_row, c_row = h_i[rows, :], c_i[rows, :]
            parts, total = [], None
            for k in range(TILE_J // LANES):
                m0 = pl.multiple_of(col_at + j0 + k * LANES, LANES)
                h_col = cols[1:2, pl.ds(m0, LANES)]
                c_col = cols[0:1, pl.ds(m0, LANES)]
                arg = jnp.minimum(gram[:, k * LANES:(k + 1) * LANES] * (2.0 * scale) - h_row - h_col, 0.0)
                w = jnp.exp2(arg) * c_row * c_col
                if diag:
                    row_id = lax.broadcasted_iota(jnp.int32, (TILE_I, LANES), 0) + i * TILE_I
                    col_id = lax.broadcasted_iota(jnp.int32, (TILE_I, LANES), 1) + (j0 + k * LANES)
                    w = jnp.where(row_id == col_id, 0.0, w)
                total = w if total is None else total + w
                parts.append(w.astype(jnp.bfloat16))
            s_ref[rows, :] += total
            t_ref[rows, :] += jnp.dot(jnp.concatenate(parts, axis=1), x_col, preferred_element_type=jnp.float32)
            return carry

        return lax.fori_loop(0, n_j, col_step, carry)

    lax.fori_loop(0, n_i, row_step, 0)


def pair_kernel(n_sets, chunks, first, scale, *refs):
    refs = list(refs)
    counts, order = refs[:2]
    meta = refs[2]
    refs = refs[3:]
    x_rows = [refs[3 * k] for k in range(n_sets)]
    h_rows = [refs[3 * k + 1] for k in range(n_sets)]
    c_rows = [refs[3 * k + 2] for k in range(n_sets)]
    refs = refs[3 * n_sets:]
    x_cols = refs[:len(chunks)]
    outs = refs[-2 * n_sets:]
    if first:
        for out in outs:
            out[...] = jnp.zeros_like(out)
    own, partner = order[0], order[order.shape[0] // 2]
    row_blocks = [own, partner][:n_sets]
    for x_col, (slot, start, size, diag) in zip(x_cols, chunks):
        block = order[slot]
        col_count = jnp.clip(counts[block] - start, 0, size)
        for k in range(n_sets):
            pair_tiles(counts[row_blocks[k]], col_count, x_rows[k], h_rows[k], c_rows[k], x_col, start, meta.at[block],
                       scale, outs[2 * k], outs[2 * k + 1], diag and k == 0)


def pair_call(counts, order, meta, rows, chunks, sums, scale, name):
    block_rows, width = rows[0][0].shape
    first = sums is None
    n_sets = len(rows)
    spec = tuple((slot, start, x.shape[0], diag) for x, slot, start, diag in chunks)
    args = [counts, order, meta] + [a for r in rows for a in r] + [c[0] for c in chunks]
    aliases = {}
    if not first:
        for k, pair in enumerate(sums):
            for m, a in enumerate(pair):
                aliases[len(args)] = 2 * k + m
                args.append(a)
    n_cols = sum(c[2] for c in spec)
    pairs = n_sets * block_rows * n_cols
    outs = pl.pallas_call(
        functools.partial(pair_kernel, n_sets, spec, first, scale),
        out_shape=[pltpu.VMEM((block_rows, w), jnp.float32) for _ in range(n_sets) for w in (width, LANES)],
        in_specs=[SMEM_SPEC, SMEM_SPEC] + [VMEM_SPEC] * (len(args) - 2),
        out_specs=[VMEM_SPEC] * (2 * n_sets),
        input_output_aliases=aliases,
        compiler_params=pltpu.CompilerParams(vmem_limit_bytes=24 << 20),
        cost_estimate=pl.CostEstimate(flops=2 * pairs * width, bytes_accessed=1 << 20, transcendentals=pairs // 4),
        name=name,
    )(*args)
    return [(outs[2 * k], outs[2 * k + 1]) for k in range(n_sets)]


def finish_kernel(inv_len2, x_ref, t_own, s_own, t_in, s_in, f_ref, e_ref):
    s = jnp.sum(s_own[...] + s_in[...], axis=1, keepdims=True)
    f_ref[...] = (s * x_ref[...].astype(jnp.float32) - (t_own[...] + t_in[...])) * inv_len2

    @pl.when(pl.program_id(0) == 0)
    def _():
        e_ref[...] = jnp.zeros_like(e_ref)

    e_ref[...] += jnp.sum(s_own[...] + s_in[...], axis=0, keepdims=True)


def finish(x, own, incoming, inv_len2):
    block_rows, width = x.shape
    tile = min(block_rows, 512)
    wide = pl.BlockSpec((tile, width), lambda i: (i, 0))
    thin = pl.BlockSpec((tile, LANES), lambda i: (i, 0))
    return pl.pallas_call(
        functools.partial(finish_kernel, inv_len2),
        grid=(block_rows // tile,),
        out_shape=[jax.ShapeDtypeStruct((block_rows, width), jnp.float32), jax.ShapeDtypeStruct((1, LANES), jnp.float32)],
        in_specs=[wide, wide, thin, wide, thin],
        out_specs=[wide, pl.BlockSpec((1, LANES), lambda i: (0, 0))],
        name='finish',
    )(x, *own, *incoming)


def solution(mesh):
    n = mesh.shape['row']
    chips = n // 2
    ring_perm = [(p, (p + 2) % n if p % 2 == 0 else (p - 2) % n) for p in range(n)]
    swap_perm = [(p, p ^ 1) for p in range(n)]

    def per_device(positions, charges, counts):
        block_rows, width = positions.shape
        scale = math.log2(math.e) * 0.5 / width
        inv_len2 = 1.0 / width
        sizes = [block_rows // 2, block_rows // 4, block_rows // 4]
        starts = [0, block_rows // 2, 3 * (block_rows // 4)]
        me = lax.axis_index('row')
        chip, core = me // 2, me % 2

        ring = [[positions[a:a + m] for a, m in zip(starts, sizes)]]
        for hop in range(1, chips):
            ring.append([lax.ppermute(x, 'row', ring_perm) for x in ring[-1]])
        partner_pos = lax.ppermute(positions, 'row', swap_perm)
        last = [lax.ppermute(x, 'row', swap_perm) for x in ring[-1][1:]]

        live_q = jnp.where(jnp.arange(block_rows) < counts[0], charges, 0.0)
        pos_f32 = positions.astype(jnp.float32)
        half = jnp.sum(pos_f32 * pos_f32, axis=1) * scale
        mine = jnp.stack([live_q, half, jnp.broadcast_to(counts[0].astype(jnp.float32), live_q.shape), jnp.zeros_like(half)])
        meta = exchange(mine, n, 0)
        all_counts = meta[:, 2, 0].astype(jnp.int32)
        steps = jnp.arange(chips)
        even = 2 * ((chip - steps) % chips)
        odd = 2 * ((chip + steps) % chips) + 1
        order = jnp.concatenate([jnp.where(core == 0, even, odd), jnp.where(core == 0, odd, even)]).astype(jnp.int32)
        partner = meta[me ^ 1]

        def spread(v):
            return jnp.broadcast_to(v[:, None], (block_rows, LANES))

        rows = [(positions, spread(half), spread(live_q)), (partner_pos, spread(partner[1]), spread(partner[0]))]
        call = functools.partial(pair_call, all_counts, order, meta)
        sums = call(rows, [(positions, 0, 0, True)], None, scale, 'pairs_0')
        for hop in range(1, chips - 1):
            sums = call(rows, [(ring[hop][0], hop, starts[0], False)], sums, scale, f'pairs_{hop}a')
            sums = call(rows, [(ring[hop][1], hop, starts[1], False), (ring[hop][2], hop, starts[2], False)], sums, scale, f'pairs_{hop}b')
        hop = chips - 1
        sums = call(rows, [(ring[hop][0], hop, starts[0], False)], sums, scale, f'pairs_{hop}a')
        incoming = tuple(lax.ppermute(a, 'row', swap_perm) for a in sums[1])
        own = sums[:1]
        for k in (1, 2):
            own = call(rows[:1], [(ring[hop][k], hop, starts[k], False), (last[k - 1], chips + hop, starts[k], False)], own, scale,
                       f'pairs_{hop}{k}')
        forces, energy_row = finish(positions, own[0], incoming, inv_len2)
        parts = exchange(jnp.broadcast_to(energy_row, (8, LANES)), n, 1)
        energy = 0.5 * jnp.sum(parts[:, 0, :])
        return forces, energy.reshape(1)

    row_spec = P(('sys', 'row'), None)
    vec_spec = P(('sys', 'row'))
    return jax.shard_map(per_device, mesh=mesh, in_specs=(row_spec, vec_spec, vec_spec), out_specs=(row_spec, P('sys')), check_vma=False)
```

```python
import functools
import math

import jax
import jax.numpy as jnp
from jax import lax
from jax.experimental import pallas as pl
from jax.experimental.pallas import tpu as pltpu
from jax.sharding import PartitionSpec as P


LANES = 128
TILE_I = 512
TILE_J = 512
BUDGET = 20
MESH = pl.DeviceIdType.MESH
VMEM_SPEC = pl.BlockSpec(memory_space=pltpu.VMEM)


def energy_kernel(n, part_ref, out_ref, seen, send_sem, recv_sem):
    me = lax.axis_index('row')
    barrier = pltpu.get_barrier_semaphore()
    for off in range(1, n):
        pl.semaphore_signal(barrier, inc=1, device_id={'row': lax.rem(me + off, n)}, device_id_type=MESH)
    pl.semaphore_wait(barrier, n - 1)
    copies = []
    for off in range(1, n):
        copies.append(pltpu.make_async_remote_copy(
            src_ref=part_ref, dst_ref=seen.at[me], send_sem=send_sem.at[off - 1], recv_sem=recv_sem.at[off - 1],
            device_id={'row': lax.rem(me + off, n)}, device_id_type=MESH))
    for copy in copies:
        copy.start()
    for copy in copies:
        copy.wait()
    total = jnp.zeros_like(part_ref)
    for k in range(n):
        total += jnp.where(me == k, part_ref[...], seen[k])
    out_ref[0] = 0.5 * jnp.sum(total)


def total_energy(part, n):
    return pl.pallas_call(
        functools.partial(energy_kernel, n),
        out_shape=jax.ShapeDtypeStruct((1,), jnp.float32),
        in_specs=[VMEM_SPEC],
        out_specs=pl.BlockSpec(memory_space=pltpu.SMEM),
        scratch_shapes=[pltpu.VMEM((n,) + part.shape, jnp.float32), pltpu.SemaphoreType.DMA((n - 1,)), pltpu.SemaphoreType.DMA((n - 1,))],
        compiler_params=pltpu.CompilerParams(collective_id=0, has_side_effects=True),
        name='energy',
    )(part)


def exchange_kernel(n, src_ref, out_ref, send_sem, recv_sem, local_sem):
    me = lax.axis_index('row')
    barrier = pltpu.get_barrier_semaphore()
    for off in range(1, n):
        pl.semaphore_signal(barrier, inc=1, device_id={'row': lax.rem(me + off, n)}, device_id_type=MESH)
    own = pltpu.make_async_copy(src_ref, out_ref.at[me], local_sem)
    own.start()
    pl.semaphore_wait(barrier, n - 1)
    copies = []
    for off in range(1, n):
        copies.append(pltpu.make_async_remote_copy(
            src_ref=src_ref, dst_ref=out_ref.at[me], send_sem=send_sem.at[off - 1], recv_sem=recv_sem.at[off - 1],
            device_id={'row': lax.rem(me + off, n)}, device_id_type=MESH))
    for copy in copies:
        copy.start()
    own.wait()
    for copy in copies:
        copy.wait()


def exchange(src, n):
    return pl.pallas_call(
        functools.partial(exchange_kernel, n),
        out_shape=jax.ShapeDtypeStruct((n,) + src.shape, src.dtype),
        in_specs=[pl.BlockSpec(memory_space=pltpu.HBM)],
        out_specs=pl.BlockSpec(memory_space=pltpu.HBM),
        scratch_shapes=[pltpu.SemaphoreType.DMA((n - 1,)), pltpu.SemaphoreType.DMA((n - 1,)), pltpu.SemaphoreType.DMA],
        compiler_params=pltpu.CompilerParams(collective_id=1, has_side_effects=True),
        cost_estimate=pl.CostEstimate(flops=0, bytes_accessed=8 << 20, transcendentals=0),
        name='exchange',
    )(src)


def up(value, step):
    return pl.cdiv(value, step) * step


def pair_kernel(cfg, *refs):
    rows, width, n, scale = cfg['rows'], cfg['width'], cfg['n'], cfg['scale']
    metas, refs = refs[0], refs[1:]
    loads, refs = refs[:len(cfg['loads'])], refs[len(cfg['loads']):]
    if cfg['stage'] == 0:
        partner_pos, spread_h, spread_c, refs = refs[0], refs[1], refs[2], refs[3:]
    if cfg['finish']:
        incoming, refs = refs[0], refs[1:]
    if cfg['stage'] > 0:
        refs = refs[6:]
    x_row, h_row_all, c_row_all, x_col, cols, sums = refs[:6]
    gram_a, gram_b = refs[-2:]
    extra = refs[6:-2]

    me = lax.axis_index('row')
    ahead = jnp.where(lax.rem(me, 2) == 0, n - 2, 2)
    mate = me + 1 - 2 * lax.rem(me, 2)
    block_of = {'own': me, 'near': lax.rem(me + ahead, n), 'next': lax.rem(me + n - ahead, n), 'far': lax.rem(me + n // 2, n),
                'mate': mate, 'away': lax.rem(mate + n // 2, n)}
    names = []
    for stage in cfg['plan'][:cfg['stage'] + 1]:
        names += [c[0] for c in stage]
    count = {k: jnp.max(metas[block_of[k], 2:3, 0:LANES]).astype(jnp.int32) for k in ['mate'] + sorted(set(names))}
    tiles_own = pl.cdiv(count['own'], TILE_I)
    row_mate = pl.multiple_of(up(count['own'], LANES), LANES)
    tiles_both = pl.cdiv(row_mate + count['mate'], TILE_I)

    end = jnp.int32(0)
    lo = jnp.int32(0)
    for stage, chunks in enumerate(cfg['plan'][:cfg['stage'] + 1]):
        mode = cfg['modes'][stage]
        for k, (name, start, size) in enumerate(chunks):
            if stage == cfg['stage']:
                at = pl.multiple_of(end, LANES)
                x_col[pl.ds(at, size), :] = loads[k][...]
                x_col[pl.ds(pl.multiple_of(at + size, LANES), TILE_J), :] = jnp.zeros((TILE_J, width), x_col.dtype)
                cols[:, pl.ds(at, size)] = metas[block_of[name], 0:2, start:start + size]
                cols[:, pl.ds(pl.multiple_of(at + size, LANES), TILE_J)] = jnp.zeros((2, TILE_J), jnp.float32)
            end = end + up(jnp.clip(count[name] - start, 0, size), LANES)
        tiles = tiles_own if mode == 'own' else tiles_both
        have = pl.cdiv(end, TILE_J) if cfg['close'][stage] else end // TILE_J
        budget = cfg['budget'][stage]
        hi = have if budget is None else jnp.minimum(have, lo + budget // jnp.maximum(tiles, 1))
        if stage < cfg['stage']:
            lo = hi
        if cfg['close'][stage]:
            end = up(end, TILE_J)
    n_j = hi - lo
    units = n_j * tiles

    if cfg['stage'] == 0:
        sums[...] = jnp.zeros_like(sums)
        x_row[0:rows, :] = loads[0][...]
        h_row_all[0:rows, :] = spread_h[0:rows, :]
        c_row_all[0:rows, :] = spread_c[0:rows, :]
        x_row[pl.ds(row_mate, rows), :] = partner_pos[...]
        h_row_all[pl.ds(row_mate, rows), :] = spread_h[rows:, :]
        c_row_all[pl.ds(row_mate, rows), :] = spread_c[rows:, :]

    def decode(unit):
        at = jnp.minimum(unit, units - 1)
        j = at // tiles
        return (at - j * tiles) * TILE_I, (j + lo) * TILE_J, jnp.where(unit < units, (j + lo) * TILE_J, cfg['null'])

    def aligned(pos):
        row, col, meta = pos
        return (pl.ds(pl.multiple_of(row, TILE_I), TILE_I), pl.ds(pl.multiple_of(col, TILE_J), TILE_J), pl.multiple_of(meta, TILE_J))

    def gram(pos, out):
        row, col, _ = aligned(pos)
        out[...] = lax.dot_general(x_row[row, :], x_col[col, :], (((1,), (1,)), ((), ())), preferred_element_type=jnp.float32)

    def weigh(pos, prod):
        row, col, meta = aligned(pos)
        h_row, c_row = h_row_all[row, :], c_row_all[row, :]
        parts, total = [], None
        for k in range(TILE_J // LANES):
            at = pl.ds(pl.multiple_of(meta + k * LANES, LANES), LANES)
            arg = jnp.minimum(prod[:, k * LANES:(k + 1) * LANES] * (2.0 * scale) - h_row - cols[1:2, at], 0.0)
            w = jnp.exp2(arg) * c_row * cols[0:1, at]
            if cfg['stage'] == 0:
                off = pos[1] + k * LANES
                off = jnp.where(off < row_mate, off - pos[0], 1 << 20)
                w = jnp.where(lax.broadcasted_iota(jnp.int32, (TILE_I, LANES), 0) - lax.broadcasted_iota(jnp.int32, (TILE_I, LANES), 1) == off, 0.0, w)
            total = w if total is None else total + w
            parts.append(w.astype(jnp.bfloat16))
        sums[row, width:] += total
        sums[row, :width] += jnp.dot(jnp.concatenate(parts, axis=1), x_col[col, :], preferred_element_type=jnp.float32)

    @pl.when(units > 0)
    def _():
        first = decode(0)
        gram(first, gram_a)

        def step(p, pos):
            mid = decode(2 * p + 1)
            gram(mid, gram_b)
            weigh(pos, gram_a)
            nxt = decode(2 * p + 2)
            gram(nxt, gram_a)
            weigh(mid, gram_b)
            return nxt

        lax.fori_loop(0, pl.cdiv(units, 2), step, first)

    if cfg['split']:
        extra[0][...] = sums[pl.ds(row_mate, rows), :]
    if cfg['finish']:
        force, part = extra
        part[...] = jnp.zeros_like(part)

        def tile(i, carry):
            at = pl.ds(pl.multiple_of(i * TILE_I, TILE_I), TILE_I)
            live = lax.broadcasted_iota(jnp.int32, (TILE_I, LANES), 0) + i * TILE_I < count['own']
            lanes = jnp.where(live, sums[at, width:] + incoming[at, width:], 0.0)
            x = x_row[at, :].astype(jnp.float32)
            value = (jnp.sum(lanes, axis=1, keepdims=True) * x - (sums[at, :width] + incoming[at, :width])) * cfg['inv_len2']
            force[at, :] = jnp.where(live[:, :1], value, 0.0)
            part[...] += jnp.sum(lanes.reshape(TILE_I // 8, 8, LANES), axis=0)
            return carry

        lax.fori_loop(0, rows // TILE_I, tile, 0)


def pair_call(stage, n, plan, modes, close, budget, metas, chunks, state, first=None, incoming=None, split=False):
    width = chunks[0].shape[1]
    rows = metas.shape[2]
    tall = 2 * rows + TILE_I
    null = up(sum(c[2] for s in plan for c in s), TILE_J) + (len(plan) + 1) * TILE_J
    cfg = dict(rows=rows, width=width, n=n, null=null, stage=stage, plan=plan, modes=modes, close=close, budget=budget, loads=chunks,
               finish=incoming is not None, split=split, scale=math.log2(math.e) * 0.5 / width, inv_len2=1.0 / width)
    args = [metas] + list(chunks)
    if stage == 0:
        args += list(first)
    if incoming is not None:
        args.append(incoming)
    aliases = {}
    if stage > 0:
        for k, a in enumerate(state):
            aliases[len(args)] = k
            args.append(a)
    out_shape = [pltpu.VMEM((tall, width), jnp.bfloat16), pltpu.VMEM((tall, LANES), jnp.float32), pltpu.VMEM((tall, LANES), jnp.float32),
                 pltpu.VMEM((null, width), jnp.bfloat16), pltpu.VMEM((2, null + TILE_J), jnp.float32), pltpu.VMEM((tall, width + LANES), jnp.float32)]
    if split:
        out_shape.append(jax.ShapeDtypeStruct((rows, width + LANES), jnp.float32))
    if incoming is not None:
        out_shape += [jax.ShapeDtypeStruct((rows, width), jnp.float32), pltpu.VMEM((8, LANES), jnp.float32)]
    outs = pl.pallas_call(
        functools.partial(pair_kernel, cfg),
        out_shape=out_shape,
        in_specs=[VMEM_SPEC] * len(args),
        out_specs=[VMEM_SPEC] * len(out_shape),
        input_output_aliases=aliases,
        scratch_shapes=[pltpu.VMEM((TILE_I, TILE_J), jnp.float32)] * 2,
        compiler_params=pltpu.CompilerParams(vmem_limit_bytes=18 << 20),
        cost_estimate=pl.CostEstimate(flops=1 << 30, bytes_accessed=1 << 20, transcendentals=0),
    )(*args)
    return list(outs[:6]), outs[6:]


def solution(mesh):
    n = mesh.shape['row']
    forth = [(p, (p + 2) % n if p % 2 == 0 else (p - 2) % n) for p in range(n)]
    back = [(b, a) for a, b in forth]
    swap = [(p, p ^ 1) for p in range(n)]

    def move(x, perm):
        return lax.ppermute(x, 'row', perm)

    def body(positions, charges, counts):
        block_rows, width = positions.shape
        half_rows = block_rows // 2
        scale = math.log2(math.e) * 0.5 / width

        live_q = jnp.where(jnp.arange(block_rows) < counts[0], charges, 0.0)
        pos_f32 = positions.astype(jnp.float32)
        half = jnp.sum(pos_f32 * pos_f32, axis=1) * scale
        meta = jnp.stack([live_q, half, jnp.broadcast_to(counts[0].astype(jnp.float32), live_q.shape), jnp.zeros_like(half)])
        metas = exchange(meta, n)
        mate = metas[lax.axis_index('row') ^ 1]

        top, bottom = positions[:half_rows], positions[half_rows:]
        mate_pos = move(positions, swap)
        near_a, next_a = move(top, forth), move(top, back)
        near_b, next_b = move(bottom, forth), move(bottom, back)
        far_a, far_b = move(near_a, forth), move(near_b, forth)
        away_a, away_b = move(far_a, swap), move(far_b, swap)

        def spread(k):
            return jnp.broadcast_to(jnp.concatenate([meta[k], mate[k]])[:, None], (2 * block_rows, LANES))

        def upper(name):
            return name, 0, half_rows

        def lower(name):
            return name, half_rows, block_rows - half_rows

        plan = [[('own', 0, block_rows)], [upper('near'), upper('next')], [lower('near'), lower('next')],
                [upper('far')], [lower('far'), upper('away')], [lower('away')]]
        arrays = [[positions], [near_a, next_a], [near_b, next_b], [far_a], [far_b, away_a], [away_b]]
        modes = ['both', 'both', 'both', 'own', 'own', 'own']
        close = [True, False, True, False, False, True]
        budget = [None, BUDGET, None, None, None, None]
        state = None
        for stage in range(len(plan)):
            state, out = pair_call(stage, n, plan, modes, close, budget, metas, arrays[stage], state,
                                   first=(mate_pos, spread(1), spread(0)) if stage == 0 else None,
                                   incoming=incoming if stage == len(plan) - 1 else None, split=stage == 2)
            if stage == 2:
                incoming = move(out[0], swap)
        forces, part = out
        return forces, total_energy(part, n)

    row_spec = P(('sys', 'row'), None)
    vec_spec = P(('sys', 'row'))
    step = jax.shard_map(body, mesh=mesh, in_specs=(row_spec, vec_spec, vec_spec), out_specs=(row_spec, P('sys')), check_vma=False)

    def program(positions, charges, counts):
        jax.eval_shape(step, positions, charges, counts)
        return step(positions, charges, counts)

    return program
```

```python
import functools
import math

import jax
import jax.numpy as jnp
from jax import lax
from jax.experimental import pallas as pl
from jax.experimental.pallas import tpu as pltpu
from jax.sharding import PartitionSpec as P


LANES = 128
TILE_I = 256
TILE_J = 512
UNROLL = 4
BUDGET = 38
VMEM_MB = (8, 6, 9, 6, 6, 12)
MESH = pl.DeviceIdType.MESH
VMEM_SPEC = pl.BlockSpec(memory_space=pltpu.VMEM)


def energy_kernel(n, part_ref, out_ref, seen, send_sem, recv_sem):
    me = lax.axis_index('row')
    barrier = pltpu.get_barrier_semaphore()
    for off in range(1, n):
        pl.semaphore_signal(barrier, inc=1, device_id={'row': lax.rem(me + off, n)}, device_id_type=MESH)
    pl.semaphore_wait(barrier, n - 1)
    copies = []
    for off in range(1, n):
        copies.append(pltpu.make_async_remote_copy(
            src_ref=part_ref, dst_ref=seen.at[me], send_sem=send_sem.at[off - 1], recv_sem=recv_sem.at[off - 1],
            device_id={'row': lax.rem(me + off, n)}, device_id_type=MESH))
    for copy in copies:
        copy.start()
    for copy in copies:
        copy.wait()
    total = jnp.zeros_like(part_ref)
    for k in range(n):
        total += jnp.where(me == k, part_ref[...], seen[k])
    out_ref[0] = 0.5 * jnp.sum(total)


def total_energy(part, n):
    return pl.pallas_call(
        functools.partial(energy_kernel, n),
        out_shape=jax.ShapeDtypeStruct((1,), jnp.float32),
        in_specs=[VMEM_SPEC],
        out_specs=pl.BlockSpec(memory_space=pltpu.SMEM),
        scratch_shapes=[pltpu.VMEM((n,) + part.shape, jnp.float32), pltpu.SemaphoreType.DMA((n - 1,)), pltpu.SemaphoreType.DMA((n - 1,))],
        compiler_params=pltpu.CompilerParams(collective_id=0, has_side_effects=True),
        name='energy',
    )(part)


def exchange_kernel(n, scale, pos_ref, q_ref, count_ref, top_ref, bottom_ref, mate_ref, meta_out, x_buf, meta, send_sem, recv_sem, local_sem, pos_sem):
    rows, width = pos_ref.shape
    me = lax.axis_index('row')
    mate = me + 1 - 2 * lax.rem(me, 2)
    barrier = pltpu.get_barrier_semaphore()
    for off in range(1, n):
        pl.semaphore_signal(barrier, inc=1, device_id={'row': lax.rem(me + off, n)}, device_id_type=MESH)
    load = pltpu.make_async_copy(pos_ref, x_buf, local_sem.at[0])
    load.start()
    load.wait()
    halves = [pltpu.make_async_copy(x_buf.at[pl.ds(0, rows // 2), :], top_ref, local_sem.at[0]),
              pltpu.make_async_copy(x_buf.at[pl.ds(rows // 2, rows // 2), :], bottom_ref, local_sem.at[1])]
    for copy in halves:
        copy.start()
    lane = lax.broadcasted_iota(jnp.int32, (1, LANES), 1)
    for b in range(rows // LANES):
        x = x_buf[b * LANES:(b + 1) * LANES, :].astype(jnp.float32)
        x = x * x
        part = x[:, :LANES]
        for k in range(1, width // LANES):
            part = part + x[:, k * LANES:(k + 1) * LANES]
        meta[1, b:b + 1, :] = jnp.sum(part.T, axis=0, keepdims=True) * scale
        meta[0, b:b + 1, :] = jnp.where(lane + b * LANES < count_ref[0], q_ref[b:b + 1, :], 0.0)
    meta[2] = jnp.full(meta.shape[1:], count_ref[0], jnp.int32).astype(jnp.float32)
    for copy in halves:
        copy.wait()
    pl.semaphore_wait(barrier, n - 1)
    copies = [pltpu.make_async_remote_copy(src_ref=x_buf, dst_ref=mate_ref, send_sem=pos_sem.at[0], recv_sem=pos_sem.at[1],
                                           device_id={'row': mate}, device_id_type=MESH)]
    for off in range(1, n):
        copies.append(pltpu.make_async_remote_copy(
            src_ref=meta, dst_ref=meta_out.at[me], send_sem=send_sem.at[off - 1], recv_sem=recv_sem.at[off - 1],
            device_id={'row': lax.rem(me + off, n)}, device_id_type=MESH))
    for copy in copies:
        copy.start()
    own = pltpu.make_async_copy(meta, meta_out.at[me], local_sem.at[2])
    own.start()
    own.wait()
    for copy in copies:
        copy.wait()


def exchange(positions, charges, counts, n):
    rows, width = positions.shape
    hbm = pl.BlockSpec(memory_space=pltpu.HBM)
    groups = rows // LANES
    half = jax.ShapeDtypeStruct((rows // 2, width), positions.dtype)
    return pl.pallas_call(
        functools.partial(exchange_kernel, n, math.log2(math.e) * 0.5 / width),
        out_shape=[half, half, jax.ShapeDtypeStruct((rows, width), positions.dtype), jax.ShapeDtypeStruct((n, 3, groups, LANES), jnp.float32)],
        in_specs=[hbm, VMEM_SPEC, pl.BlockSpec(memory_space=pltpu.SMEM)],
        out_specs=[hbm] * 4,
        scratch_shapes=[pltpu.VMEM((rows, width), positions.dtype), pltpu.VMEM((3, groups, LANES), jnp.float32),
                        pltpu.SemaphoreType.DMA((n - 1,)), pltpu.SemaphoreType.DMA((n - 1,)), pltpu.SemaphoreType.DMA((3,)),
                        pltpu.SemaphoreType.DMA((2,))],
        compiler_params=pltpu.CompilerParams(collective_id=1, has_side_effects=True, vmem_limit_bytes=6 << 20),
        cost_estimate=pl.CostEstimate(flops=0, bytes_accessed=8 << 20, transcendentals=0),
        name='exchange',
    )(positions, charges.reshape(groups, LANES), counts)


def up(value, step):
    return pl.cdiv(value, step) * step


def pair_kernel(cfg, *refs):
    rows, width, n, scale = cfg['rows'], cfg['width'], cfg['n'], cfg['scale']
    metas, refs = refs[0], refs[1:]
    loads, refs = refs[:len(cfg['loads'])], refs[len(cfg['loads']):]
    if cfg['stage'] == 0:
        mate_pos, refs = refs[0], refs[1:]
    if cfg['finish']:
        incoming, refs = refs[0], refs[1:]
    if cfg['stage'] > 0:
        refs = refs[7:]
    x_row, h_row_all, c_row_all, x_col, cols, pulls, sums = refs[:7]
    gram_a, gram_b = refs[-2:]
    extra = refs[7:-2]

    me = lax.axis_index('row')
    ahead = jnp.where(lax.rem(me, 2) == 0, n - 2, 2)
    mate = me + 1 - 2 * lax.rem(me, 2)
    block_of = {'own': me, 'near': lax.rem(me + ahead, n), 'next': lax.rem(me + n - ahead, n), 'far': lax.rem(me + n // 2, n),
                'mate': mate, 'away': lax.rem(mate + n // 2, n)}
    names = []
    for stage in cfg['plan'][:cfg['stage'] + 1]:
        names += [c[0] for c in stage]
    count = {k: jnp.max(metas[block_of[k], 2, 0:1, :]).astype(jnp.int32) for k in ['mate'] + sorted(set(names))}
    tiles_own = pl.cdiv(count['own'], TILE_I)
    row_mate = pl.multiple_of(up(count['own'], LANES), LANES)
    tiles_both = pl.cdiv(row_mate + count['mate'], TILE_I)

    end = jnp.int32(0)
    lo = jnp.int32(0)
    for stage, chunks in enumerate(cfg['plan'][:cfg['stage'] + 1]):
        mode = cfg['modes'][stage]
        for k, (name, start, size) in enumerate(chunks):
            if stage == cfg['stage']:
                at = pl.multiple_of(end, LANES)
                x_col[pl.ds(at, size), :] = loads[k][...]
                x_col[pl.ds(pl.multiple_of(at + size, LANES), TILE_J), :] = jnp.zeros((TILE_J, width), x_col.dtype)
                for g in range(size // LANES):
                    for m in range(2):
                        cols[m:m + 1, pl.ds(pl.multiple_of(at + g * LANES, LANES), LANES)] = metas[block_of[name], m, pl.ds(start // LANES + g, 1), :]
                cols[:, pl.ds(pl.multiple_of(at + size, LANES), TILE_J)] = jnp.zeros((2, TILE_J), jnp.float32)
            end = end + up(jnp.clip(count[name] - start, 0, size), LANES)
        tiles = tiles_own if mode == 'own' else tiles_both
        have = pl.cdiv(end, TILE_J) if cfg['close'][stage] else end // TILE_J
        budget = cfg['budget'][stage]
        hi = have if budget is None else jnp.minimum(have, lo + budget // jnp.maximum(tiles, 1))
        if stage < cfg['stage']:
            lo = hi
        if cfg['close'][stage]:
            end = up(end, TILE_J)
    n_j = hi - lo
    units = n_j * tiles

    if cfg['stage'] == 0:
        sums[...] = jnp.zeros_like(sums)
        pulls[...] = jnp.zeros_like(pulls)
        for name, row0, src in (('own', 0, loads[0]), ('mate', row_mate, mate_pos)):
            x_row[pl.ds(row0, rows), :] = src[...]
            for g in range(rows // LANES):
                at = pl.ds(pl.multiple_of(row0 + g * LANES, LANES), LANES)
                c_row_all[at, :] = jnp.broadcast_to(metas[block_of[name], 0, g:g + 1, :], (LANES, LANES)).T
                h_row_all[at, :] = jnp.broadcast_to(metas[block_of[name], 1, g:g + 1, :], (LANES, LANES)).T

    def decode(unit):
        at = jnp.minimum(unit, units - 1)
        j = at // tiles
        return (at - j * tiles) * TILE_I, (j + lo) * TILE_J, jnp.where(unit < units, (j + lo) * TILE_J, cfg['null'])

    def aligned(pos):
        row, col, meta = pos
        return (pl.ds(pl.multiple_of(row, TILE_I), TILE_I), pl.ds(pl.multiple_of(col, TILE_J), TILE_J), pl.multiple_of(meta, TILE_J))

    def gram(pos, out):
        row, col, _ = aligned(pos)
        out[...] = lax.dot_general(x_row[row, :], x_col[col, :], (((1,), (1,)), ((), ())), preferred_element_type=jnp.float32)

    def weigh(pos, prod):
        row, col, meta = aligned(pos)
        h_row, c_row = h_row_all[row, :], c_row_all[row, :]
        parts, total = [], None
        for k in range(TILE_J // LANES):
            at = pl.ds(pl.multiple_of(meta + k * LANES, LANES), LANES)
            arg = jnp.minimum(prod[:, k * LANES:(k + 1) * LANES] * (2.0 * scale) - h_row - cols[1:2, at], 0.0)
            w = jnp.exp2(arg) * c_row * cols[0:1, at]
            if cfg['stage'] == 0:
                off = pos[1] + k * LANES
                off = jnp.where(off < row_mate, off - pos[0], 1 << 20)
                w = jnp.where(lax.broadcasted_iota(jnp.int32, (TILE_I, LANES), 0) - lax.broadcasted_iota(jnp.int32, (TILE_I, LANES), 1) == off, 0.0, w)
            total = w if total is None else total + w
            parts.append(w.astype(jnp.bfloat16))
        sums[row, :] += total
        pulls[:width, row] += lax.dot_general(x_col[col, :], jnp.concatenate(parts, axis=1), (((0,), (1,)), ((), ())),
                                              preferred_element_type=jnp.float32)

    @pl.when(units > 0)
    def _():
        first = decode(0)
        gram(first, gram_a)

        def step(p, pos):
            for k in range(UNROLL):
                nxt = decode(UNROLL * p + k + 1)
                gram(nxt, (gram_a, gram_b)[(k + 1) % 2])
                weigh(pos, (gram_a, gram_b)[k % 2])
                pos = nxt
            return pos

        lax.fori_loop(0, pl.cdiv(units, UNROLL), step, first)

    if cfg['split']:
        for g in range(rows // LANES):
            at = pl.ds(pl.multiple_of(row_mate + g * LANES, LANES), LANES)
            pulls[width:, at] = jnp.sum(sums[at, :].T.reshape(LANES // 8, 8, LANES), axis=0)
        extra[0][...] = pulls[:, pl.ds(row_mate, rows)]
    if cfg['finish']:
        force, part = extra
        part[...] = jnp.zeros_like(part)

        def tile(i, carry):
            at = pl.ds(pl.multiple_of(i * LANES, LANES), LANES)
            live = lax.broadcasted_iota(jnp.int32, (LANES, LANES), 0) + i * LANES < count['own']
            lanes = jnp.where(live, sums[at, :], 0.0)
            inc = jnp.where(lax.broadcasted_iota(jnp.int32, (8, LANES), 1) + i * LANES < count['own'], incoming[width:, at], 0.0)
            total = jnp.sum(lanes, axis=1, keepdims=True) + jnp.broadcast_to(jnp.sum(inc, axis=0, keepdims=True), (LANES, LANES)).T
            for k in range(width // LANES):
                d = pl.ds(k * LANES, LANES)
                value = total * x_row[at, d].astype(jnp.float32) - (pulls[d, at] + incoming[d, at]).T
                force[at, d] = jnp.where(live, value * cfg['inv_len2'], 0.0)
            part[...] += jnp.sum(lanes.reshape(LANES // 8, 8, LANES), axis=0) + inc
            return carry

        lax.fori_loop(0, rows // LANES, tile, 0)


def pair_call(stage, n, plan, modes, close, budget, metas, chunks, state, first=None, incoming=None, split=False):
    width = chunks[0].shape[1]
    rows = metas.shape[2] * metas.shape[3]
    tall = 2 * rows + TILE_I
    null = up(sum(c[2] for s in plan for c in s), TILE_J) + (len(plan) + 1) * TILE_J
    cfg = dict(rows=rows, width=width, n=n, null=null, stage=stage, plan=plan, modes=modes, close=close, budget=budget, loads=chunks,
               finish=incoming is not None, split=split, scale=math.log2(math.e) * 0.5 / width, inv_len2=1.0 / width)
    args = [metas] + list(chunks)
    if stage == 0:
        args += list(first)
    if incoming is not None:
        args.append(incoming)
    aliases = {}
    if stage > 0:
        for k, a in enumerate(state):
            aliases[len(args)] = k
            args.append(a)
    out_shape = [pltpu.VMEM((tall, width), jnp.bfloat16), pltpu.VMEM((tall, LANES), jnp.float32), pltpu.VMEM((tall, LANES), jnp.float32),
                 pltpu.VMEM((null, width), jnp.bfloat16), pltpu.VMEM((2, null + TILE_J), jnp.float32), pltpu.VMEM((width + 8, tall), jnp.float32),
                 pltpu.VMEM((tall, LANES), jnp.float32)]
    if split:
        out_shape.append(jax.ShapeDtypeStruct((width + 8, rows), jnp.float32))
    if incoming is not None:
        out_shape += [jax.ShapeDtypeStruct((rows, width), jnp.float32), pltpu.VMEM((8, LANES), jnp.float32)]
    outs = pl.pallas_call(
        functools.partial(pair_kernel, cfg),
        out_shape=out_shape,
        in_specs=[VMEM_SPEC] * len(args),
        out_specs=[VMEM_SPEC] * len(out_shape),
        input_output_aliases=aliases,
        scratch_shapes=[pltpu.VMEM((TILE_I, TILE_J), jnp.float32)] * 2,
        compiler_params=pltpu.CompilerParams(vmem_limit_bytes=(VMEM_MB[stage]) << 20),
        cost_estimate=pl.CostEstimate(flops=1 << 30, bytes_accessed=1 << 20, transcendentals=0),
    )(*args)
    return list(outs[:7]), outs[7:]


def solution(mesh):
    n = mesh.shape['row']
    forth = [(p, (p + 2) % n if p % 2 == 0 else (p - 2) % n) for p in range(n)]
    back = [(b, a) for a, b in forth]
    swap = [(p, p ^ 1) for p in range(n)]

    def move(x, perm):
        return lax.ppermute(x, 'row', perm)

    def body(positions, charges, counts):
        block_rows, _ = positions.shape
        half_rows = block_rows // 2

        top, bottom, mate_pos, metas = exchange(positions, charges, counts, n)
        near_a, next_a = move(top, forth), move(top, back)
        near_b, next_b = move(bottom, forth), move(bottom, back)
        far_a, far_b = move(near_a, forth), move(near_b, forth)
        away_a, away_b = move(far_a, swap), move(far_b, swap)

        def upper(name):
            return name, 0, half_rows

        def lower(name):
            return name, half_rows, block_rows - half_rows

        plan = [[('own', 0, block_rows)], [upper('near'), upper('next')], [lower('near'), lower('next')],
                [upper('far')], [lower('far'), upper('away')], [lower('away')]]
        arrays = [[positions], [near_a, next_a], [near_b, next_b], [far_a], [far_b, away_a], [away_b]]
        modes = ['both', 'both', 'both', 'own', 'own', 'own']
        close = [True, False, True, False, False, True]
        budget = [None, BUDGET, None, None, None, None]
        state = None
        for stage in range(len(plan)):
            state, out = pair_call(stage, n, plan, modes, close, budget, metas, arrays[stage], state,
                                   first=(mate_pos,) if stage == 0 else None,
                                   incoming=incoming if stage == len(plan) - 1 else None, split=stage == 2)
            if stage == 2:
                incoming = move(out[0], swap)
        forces, part = out
        return forces, total_energy(part, n)

    row_spec = P(('sys', 'row'), None)
    vec_spec = P(('sys', 'row'))
    step = jax.shard_map(body, mesh=mesh, in_specs=(row_spec, vec_spec, vec_spec), out_specs=(row_spec, P('sys')), check_vma=False)

    def program(positions, charges, counts):
        jax.eval_shape(step, positions, charges, counts)
        return step(positions, charges, counts)

    return program
```

```python
import functools
import math

import jax
import jax.numpy as jnp
from jax import lax
from jax.experimental import pallas as pl
from jax.experimental.pallas import tpu as pltpu
from jax.sharding import PartitionSpec as P


LANES = 128
TILE_I = 256
TILE_J = 512
UNROLL = 4
BUDGET = 38
VMEM_MB = (5, 6, 9, 5, 5, 5, 11)
MESH = pl.DeviceIdType.MESH
VMEM_SPEC = pl.BlockSpec(memory_space=pltpu.VMEM)


def energy_kernel(n, part_hbm, out_ref, seen, part_ref, send_sem, recv_sem, local_sem):
    me = lax.axis_index('row')
    barrier = pltpu.get_barrier_semaphore()
    for off in range(1, n):
        pl.semaphore_signal(barrier, inc=1, device_id={'row': lax.rem(me + off, n)}, device_id_type=MESH)
    load = pltpu.make_async_copy(part_hbm, part_ref, local_sem)
    load.start()
    load.wait()
    pl.semaphore_wait(barrier, n - 1)
    copies = []
    for off in range(1, n):
        copies.append(pltpu.make_async_remote_copy(
            src_ref=part_ref, dst_ref=seen.at[me], send_sem=send_sem.at[off - 1], recv_sem=recv_sem.at[off - 1],
            device_id={'row': lax.rem(me + off, n)}, device_id_type=MESH))
    for copy in copies:
        copy.start()
    for copy in copies:
        copy.wait()
    total = jnp.zeros(part_ref.shape, jnp.float32)
    for k in range(n):
        total += jnp.where(me == k, part_ref[...], seen[k])
    out_ref[0] = 0.5 * jnp.sum(total)


def total_energy(part, n):
    return pl.pallas_call(
        functools.partial(energy_kernel, n),
        out_shape=jax.ShapeDtypeStruct((1,), jnp.float32),
        in_specs=[pl.BlockSpec(memory_space=pltpu.HBM)],
        out_specs=pl.BlockSpec(memory_space=pltpu.SMEM),
        scratch_shapes=[pltpu.VMEM((n,) + part.shape, jnp.float32), pltpu.VMEM(part.shape, jnp.float32), pltpu.SemaphoreType.DMA((n - 1,)),
                        pltpu.SemaphoreType.DMA((n - 1,)), pltpu.SemaphoreType.DMA],
        compiler_params=pltpu.CompilerParams(collective_id=0, has_side_effects=True),
        name='energy',
    )(part)


def exchange_kernel(n, scale, pos_ref, q_ref, count_ref, top_ref, bottom_ref, meta_out, x_buf, meta, send_sem, recv_sem, local_sem):
    rows, width = pos_ref.shape
    me = lax.axis_index('row')
    barrier = pltpu.get_barrier_semaphore()
    for off in range(1, n):
        pl.semaphore_signal(barrier, inc=1, device_id={'row': lax.rem(me + off, n)}, device_id_type=MESH)
    load = pltpu.make_async_copy(pos_ref, x_buf, local_sem.at[0])
    load.start()
    load.wait()
    halves = [pltpu.make_async_copy(x_buf.at[pl.ds(0, rows // 2), :], top_ref, local_sem.at[0]),
              pltpu.make_async_copy(x_buf.at[pl.ds(rows // 2, rows // 2), :], bottom_ref, local_sem.at[1])]
    for copy in halves:
        copy.start()
    lane = lax.broadcasted_iota(jnp.int32, (1, LANES), 1)
    for b in range(rows // LANES):
        x = x_buf[b * LANES:(b + 1) * LANES, :].astype(jnp.float32)
        x = x * x
        part = x[:, :LANES]
        for k in range(1, width // LANES):
            part = part + x[:, k * LANES:(k + 1) * LANES]
        meta[1, b:b + 1, :] = jnp.sum(part.T, axis=0, keepdims=True) * scale
        meta[0, b:b + 1, :] = jnp.where(lane + b * LANES < count_ref[0], q_ref[b:b + 1, :], 0.0)
    meta[2] = jnp.full(meta.shape[1:], count_ref[0], jnp.int32).astype(jnp.float32)
    pl.semaphore_wait(barrier, n - 1)
    copies = []
    for off in range(1, n):
        copies.append(pltpu.make_async_remote_copy(
            src_ref=meta, dst_ref=meta_out.at[me], send_sem=send_sem.at[off - 1], recv_sem=recv_sem.at[off - 1],
            device_id={'row': lax.rem(me + off, n)}, device_id_type=MESH))
    for copy in copies:
        copy.start()
    own = pltpu.make_async_copy(meta, meta_out.at[me], local_sem.at[2])
    own.start()
    own.wait()
    for copy in halves + copies:
        copy.wait()


def exchange(positions, charges, counts, n):
    rows, width = positions.shape
    hbm = pl.BlockSpec(memory_space=pltpu.HBM)
    groups = rows // LANES
    half = jax.ShapeDtypeStruct((rows // 2, width), positions.dtype)
    return pl.pallas_call(
        functools.partial(exchange_kernel, n, math.log2(math.e) * 0.5 / width),
        out_shape=[half, half, jax.ShapeDtypeStruct((n, 3, groups, LANES), jnp.float32)],
        in_specs=[hbm, VMEM_SPEC, pl.BlockSpec(memory_space=pltpu.SMEM)],
        out_specs=[hbm] * 3,
        scratch_shapes=[pltpu.VMEM((rows, width), positions.dtype), pltpu.VMEM((3, groups, LANES), jnp.float32),
                        pltpu.SemaphoreType.DMA((n - 1,)), pltpu.SemaphoreType.DMA((n - 1,)), pltpu.SemaphoreType.DMA((3,))],
        compiler_params=pltpu.CompilerParams(collective_id=1, has_side_effects=True, vmem_limit_bytes=6 << 20),
        cost_estimate=pl.CostEstimate(flops=0, bytes_accessed=8 << 20, transcendentals=0),
        name='exchange',
    )(positions, charges.reshape(groups, LANES), counts)


def up(value, step):
    return pl.cdiv(value, step) * step


def pair_kernel(cfg, *refs):
    rows, width, n, scale = cfg['rows'], cfg['width'], cfg['n'], cfg['scale']
    metas, refs = refs[0], refs[1:]
    loads, refs = refs[:len(cfg['loads'])], refs[len(cfg['loads']):]
    if cfg['stage'] == 0:
        mate_pos, refs = refs[0], refs[1:]
        copy_sem = refs[-3]
        refs = refs[:-3] + refs[-2:]
    if cfg['finish']:
        incoming, refs = refs[0], refs[1:]
    if cfg['stage'] > 0:
        refs = refs[7:]
    x_row, h_row_all, c_row_all, x_col, cols, pulls, sums = refs[:7]
    gram_a, gram_b = refs[-2:]
    extra = refs[7:-2]

    me = lax.axis_index('row')
    ahead = jnp.where(lax.rem(me, 2) == 0, n - 2, 2)
    mate = me + 1 - 2 * lax.rem(me, 2)
    block_of = {'own': me, 'near': lax.rem(me + ahead, n), 'next': lax.rem(me + n - ahead, n), 'far': lax.rem(me + n // 2, n),
                'mate': mate, 'away': lax.rem(mate + n // 2, n)}
    names = []
    for stage in cfg['plan'][:cfg['stage'] + 1]:
        names += [c[0] for c in stage]
    count = {k: jnp.max(metas[block_of[k], 2, 0:1, :]).astype(jnp.int32) for k in ['mate'] + sorted(set(names))}
    tiles_own = pl.cdiv(count['own'], TILE_I)
    row_mate = pl.multiple_of(up(count['own'], LANES), LANES)
    tiles_both = pl.cdiv(row_mate + count['mate'], TILE_I)

    end = jnp.int32(0)
    lo = jnp.int32(0)
    for stage, chunks in enumerate(cfg['plan'][:cfg['stage'] + 1]):
        mode = cfg['modes'][stage]
        for k, (name, start, size) in enumerate(chunks):
            if stage == cfg['stage']:
                at = pl.multiple_of(end, LANES)
                if stage > 0:
                    x_col[pl.ds(at, size), :] = loads[k][...]
                x_col[pl.ds(pl.multiple_of(at + size, LANES), TILE_J), :] = jnp.zeros((TILE_J, width), x_col.dtype)
                for g in range(size // LANES):
                    for m in range(2):
                        cols[m:m + 1, pl.ds(pl.multiple_of(at + g * LANES, LANES), LANES)] = metas[block_of[name], m, pl.ds(start // LANES + g, 1), :]
                cols[:, pl.ds(pl.multiple_of(at + size, LANES), TILE_J)] = jnp.zeros((2, TILE_J), jnp.float32)
            end = end + up(jnp.clip(count[name] - start, 0, size), LANES)
        tiles = tiles_own if mode == 'own' else tiles_both
        have = pl.cdiv(end, TILE_J) if cfg['close'][stage] else end // TILE_J
        budget = cfg['budget'][stage]
        hi = have if budget is None else jnp.minimum(have, lo + budget // jnp.maximum(tiles, 1))
        if stage < cfg['stage']:
            lo = hi
        if cfg['close'][stage]:
            end = up(end, TILE_J)
    n_j = hi - lo
    units = n_j * tiles

    if cfg['stage'] == 0:
        copies = [pltpu.make_async_copy(loads[0], x_row.at[pl.ds(0, rows), :], copy_sem.at[0]),
                  pltpu.make_async_copy(loads[0], x_col.at[pl.ds(0, rows), :], copy_sem.at[1]),
                  pltpu.make_async_copy(mate_pos, x_row.at[pl.ds(row_mate, rows), :], copy_sem.at[2])]
        for copy in copies[:2]:
            copy.start()
        sums[...] = jnp.zeros_like(sums)
        pulls[...] = jnp.zeros_like(pulls)
        for name, row0 in (('own', 0), ('mate', row_mate)):
            for g in range(rows // LANES):
                at = pl.ds(pl.multiple_of(row0 + g * LANES, LANES), LANES)
                c_row_all[at, :] = jnp.broadcast_to(metas[block_of[name], 0, g:g + 1, :], (LANES, LANES)).T
                h_row_all[at, :] = jnp.broadcast_to(metas[block_of[name], 1, g:g + 1, :], (LANES, LANES)).T
        copies[0].wait()
        copies[2].start()
        copies[1].wait()
        copies[2].wait()

    def decode(unit):
        at = jnp.minimum(unit, units - 1)
        j = at // tiles
        return (at - j * tiles) * TILE_I, (j + lo) * TILE_J, jnp.where(unit < units, (j + lo) * TILE_J, cfg['null'])

    def aligned(pos):
        row, col, meta = pos
        return (pl.ds(pl.multiple_of(row, TILE_I), TILE_I), pl.ds(pl.multiple_of(col, TILE_J), TILE_J), pl.multiple_of(meta, TILE_J))

    def gram(pos, out):
        row, col, _ = aligned(pos)
        out[...] = lax.dot_general(x_row[row, :], x_col[col, :], (((1,), (1,)), ((), ())), preferred_element_type=jnp.float32)

    def weigh(pos, prod):
        row, col, meta = aligned(pos)
        h_row, c_row = h_row_all[row, :], c_row_all[row, :]
        parts, total = [], None
        for k in range(TILE_J // LANES):
            at = pl.ds(pl.multiple_of(meta + k * LANES, LANES), LANES)
            arg = jnp.minimum(prod[:, k * LANES:(k + 1) * LANES] * (2.0 * scale) - h_row - cols[1:2, at], 0.0)
            w = jnp.exp2(arg) * c_row * cols[0:1, at]
            if cfg['stage'] == 0:
                off = pos[1] + k * LANES
                off = jnp.where(off < row_mate, off - pos[0], 1 << 20)
                w = jnp.where(lax.broadcasted_iota(jnp.int32, (TILE_I, LANES), 0) - lax.broadcasted_iota(jnp.int32, (TILE_I, LANES), 1) == off, 0.0, w)
            total = w if total is None else total + w
            parts.append(w.astype(jnp.bfloat16))
        sums[row, :] += total
        pulls[:width, row] += lax.dot_general(x_col[col, :], jnp.concatenate(parts, axis=1), (((0,), (1,)), ((), ())),
                                              preferred_element_type=jnp.float32)

    @pl.when(units > 0)
    def _():
        first = decode(0)
        gram(first, gram_a)

        def step(p, pos):
            for k in range(UNROLL):
                nxt = decode(UNROLL * p + k + 1)
                gram(nxt, (gram_a, gram_b)[(k + 1) % 2])
                weigh(pos, (gram_a, gram_b)[k % 2])
                pos = nxt
            return pos

        lax.fori_loop(0, pl.cdiv(units, UNROLL), step, first)

    if cfg['split']:
        for g in range(rows // LANES):
            at = pl.ds(pl.multiple_of(row_mate + g * LANES, LANES), LANES)
            pulls[width:, at] = jnp.sum(sums[at, :].T.reshape(LANES // 8, 8, LANES), axis=0)
        extra[0][...] = pulls[:, pl.ds(row_mate, rows)]
    if cfg['finish']:
        force, part = extra
        part[...] = jnp.zeros_like(part)

        def tile(i, carry):
            at = pl.ds(pl.multiple_of(i * LANES, LANES), LANES)
            live = lax.broadcasted_iota(jnp.int32, (LANES, LANES), 0) + i * LANES < count['own']
            lanes = jnp.where(live, sums[at, :], 0.0)
            inc = jnp.where(lax.broadcasted_iota(jnp.int32, (8, LANES), 1) + i * LANES < count['own'], incoming[width:, at], 0.0)
            total = jnp.sum(lanes, axis=1, keepdims=True) + jnp.broadcast_to(jnp.sum(inc, axis=0, keepdims=True), (LANES, LANES)).T
            for k in range(width // LANES):
                d = pl.ds(k * LANES, LANES)
                value = total * x_row[at, d].astype(jnp.float32) - (pulls[d, at] + incoming[d, at]).T
                force[at, d] = jnp.where(live, value * cfg['inv_len2'], 0.0)
            part[...] += jnp.sum(lanes.reshape(LANES // 8, 8, LANES), axis=0) + inc
            return carry

        lax.fori_loop(0, rows // LANES, tile, 0, unroll=4)


def pair_call(stage, n, plan, modes, close, budget, metas, chunks, state, first=None, incoming=None, split=False):
    width = chunks[0].shape[1]
    rows = metas.shape[2] * metas.shape[3]
    tall = 2 * rows + TILE_I
    null = up(sum(c[2] for s in plan for c in s), TILE_J) + (len(plan) + 1) * TILE_J
    cfg = dict(rows=rows, width=width, n=n, null=null, stage=stage, plan=plan, modes=modes, close=close, budget=budget, loads=chunks,
               finish=incoming is not None, split=split, scale=math.log2(math.e) * 0.5 / width, inv_len2=1.0 / width)
    args = [metas] + list(chunks)
    if stage == 0:
        args += list(first)
    if incoming is not None:
        args.append(incoming)
    aliases = {}
    if stage > 0:
        for k, a in enumerate(state):
            aliases[len(args)] = k
            args.append(a)
    out_shape = [pltpu.VMEM((tall, width), jnp.bfloat16), pltpu.VMEM((tall, LANES), jnp.float32), pltpu.VMEM((tall, LANES), jnp.float32),
                 pltpu.VMEM((null, width), jnp.bfloat16), pltpu.VMEM((2, null + TILE_J), jnp.float32), pltpu.VMEM((width + 8, tall), jnp.float32),
                 pltpu.VMEM((tall, LANES), jnp.float32)]
    if split:
        out_shape.append(jax.ShapeDtypeStruct((width + 8, rows), jnp.float32))
    if incoming is not None:
        out_shape += [jax.ShapeDtypeStruct((rows, width), jnp.float32), jax.ShapeDtypeStruct((8, LANES), jnp.float32)]
    outs = pl.pallas_call(
        functools.partial(pair_kernel, cfg),
        out_shape=out_shape,
        in_specs=[VMEM_SPEC] + [VMEM_SPEC if stage else pl.BlockSpec(memory_space=pltpu.HBM)] * (len(args) - 1),
        out_specs=[VMEM_SPEC] * len(out_shape),
        input_output_aliases=aliases,
        scratch_shapes=([] if stage else [pltpu.SemaphoreType.DMA((3,))]) + [pltpu.VMEM((TILE_I, TILE_J), jnp.float32)] * 2,
        compiler_params=pltpu.CompilerParams(vmem_limit_bytes=(VMEM_MB[stage]) << 20),
        cost_estimate=pl.CostEstimate(flops=1 << 30, bytes_accessed=1 << 20, transcendentals=0),
    )(*args)
    return list(outs[:7]), outs[7:]


def solution(mesh):
    n = mesh.shape['row']
    forth = [(p, (p + 2) % n if p % 2 == 0 else (p - 2) % n) for p in range(n)]
    back = [(b, a) for a, b in forth]
    swap = [(p, p ^ 1) for p in range(n)]

    def move(x, perm):
        return lax.ppermute(x, 'row', perm)

    def body(positions, charges, counts):
        block_rows, _ = positions.shape
        half_rows = block_rows // 2

        mate_pos = move(positions, swap)
        top, bottom, metas = exchange(positions, charges, counts, n)
        near_a, next_a = move(top, forth), move(top, back)
        near_b, next_b = move(bottom, forth), move(bottom, back)
        far_a, far_b = move(near_a, forth), move(near_b, forth)
        away_a, away_b = move(far_a, swap), move(far_b, swap)

        def upper(name):
            return name, 0, half_rows

        def lower(name):
            return name, half_rows, block_rows - half_rows

        plan = [[('own', 0, block_rows)], [upper('near'), upper('next')], [lower('near'), lower('next')],
                [upper('far')], [upper('away')], [lower('far')], [lower('away')]]
        arrays = [[positions], [near_a, next_a], [near_b, next_b], [far_a], [away_a], [far_b], [away_b]]
        modes = ['both', 'both', 'both', 'own', 'own', 'own', 'own']
        close = [True, False, True, False, False, False, True]
        budget = [None, BUDGET, None, None, None, None, None]
        state = None
        for stage in range(len(plan)):
            state, out = pair_call(stage, n, plan, modes, close, budget, metas, arrays[stage], state,
                                   first=(mate_pos,) if stage == 0 else None,
                                   incoming=incoming if stage == len(plan) - 1 else None, split=stage == 2)
            if stage == 2:
                incoming = move(out[0], swap)
        forces, part = out
        return forces, total_energy(part, n)

    row_spec = P(('sys', 'row'), None)
    vec_spec = P(('sys', 'row'))
    step = jax.shard_map(body, mesh=mesh, in_specs=(row_spec, vec_spec, vec_spec), out_specs=(row_spec, P('sys')), check_vma=False)

    def program(positions, charges, counts):
        jax.eval_shape(step, positions, charges, counts)
        return step(positions, charges, counts)

    return program
```

```python
import functools
import math

import jax
import jax.numpy as jnp
from jax import lax
from jax.experimental import pallas as pl
from jax.experimental.pallas import tpu as pltpu
from jax.sharding import PartitionSpec as P


LANES = 128
TILE_I = 256
TILE_J = 512
UNROLL = 4
BUDGET = 38
VMEM_MB = (5, 6, 9, 5, 8, 5, 9)
MESH = pl.DeviceIdType.MESH
VMEM_SPEC = pl.BlockSpec(memory_space=pltpu.VMEM)


def energy_kernel(n, part_hbm, out_ref, seen, part_ref, send_sem, recv_sem, local_sem):
    me = lax.axis_index('row')
    barrier = pltpu.get_barrier_semaphore()
    for off in range(1, n):
        pl.semaphore_signal(barrier, inc=1, device_id={'row': lax.rem(me + off, n)}, device_id_type=MESH)
    load = pltpu.make_async_copy(part_hbm, part_ref, local_sem)
    load.start()
    load.wait()
    pl.semaphore_wait(barrier, n - 1)
    copies = []
    for off in range(1, n):
        copies.append(pltpu.make_async_remote_copy(
            src_ref=part_ref, dst_ref=seen.at[me], send_sem=send_sem.at[off - 1], recv_sem=recv_sem.at[off - 1],
            device_id={'row': lax.rem(me + off, n)}, device_id_type=MESH))
    for copy in copies:
        copy.start()
    for copy in copies:
        copy.wait()
    total = jnp.zeros(part_ref.shape, jnp.float32)
    for k in range(n):
        total += jnp.where(me == k, part_ref[...], seen[k])
    out_ref[0] = 0.5 * jnp.sum(total)


def total_energy(part, n):
    return pl.pallas_call(
        functools.partial(energy_kernel, n),
        out_shape=jax.ShapeDtypeStruct((1,), jnp.float32),
        in_specs=[pl.BlockSpec(memory_space=pltpu.HBM)],
        out_specs=pl.BlockSpec(memory_space=pltpu.SMEM),
        scratch_shapes=[pltpu.VMEM((n,) + part.shape, jnp.float32), pltpu.VMEM(part.shape, jnp.float32), pltpu.SemaphoreType.DMA((n - 1,)),
                        pltpu.SemaphoreType.DMA((n - 1,)), pltpu.SemaphoreType.DMA],
        compiler_params=pltpu.CompilerParams(collective_id=0, has_side_effects=True),
        name='energy',
    )(part)


def up(value, step):
    return pl.cdiv(value, step) * step


def spread(meta, h_rows, c_rows, row0):
    groups = meta.shape[1]
    table = jnp.concatenate([meta[0], meta[1], jnp.zeros((LANES - 2 * groups, LANES), jnp.float32)], axis=0).T
    for g in range(groups):
        at = pl.ds(pl.multiple_of(row0 + g * LANES, LANES), LANES)
        c_rows[at, :] = jnp.broadcast_to(table[:, g:g + 1], (LANES, LANES))
        h_rows[at, :] = jnp.broadcast_to(table[:, groups + g:groups + g + 1], (LANES, LANES))


def append(meta, cols, at, start, size):
    for g in range(size // LANES):
        for m in range(2):
            cols[m:m + 1, pl.ds(pl.multiple_of(at + g * LANES, LANES), LANES)] = meta[m, start // LANES + g:start // LANES + g + 1, :]
    cols[:, pl.ds(pl.multiple_of(at + size, LANES), TILE_J)] = jnp.zeros((2, TILE_J), jnp.float32)


def begin_kernel(scale, pos_ref, q_ref, count_ref, meta, x_row, h_rows, c_rows, x_col, cols, pulls, sums):
    rows, width = pos_ref.shape
    lane = lax.broadcasted_iota(jnp.int32, (LANES, LANES), 1)
    table = jnp.zeros((LANES, LANES), jnp.float32)
    for b in range(rows // LANES):
        x = pos_ref[b * LANES:(b + 1) * LANES, :].astype(jnp.float32)
        table = jnp.where(lane == b, jnp.sum(x * x, axis=1, keepdims=True), table)
        meta[0, b:b + 1, :] = jnp.where(lane[:1] + b * LANES < count_ref[0], q_ref[b:b + 1, :], 0.0)
    meta[1] = table.T[:rows // LANES, :] * scale
    meta[2] = jnp.full(meta.shape[1:], count_ref[0], jnp.int32).astype(jnp.float32)
    sums[...] = jnp.zeros_like(sums)
    pulls[...] = jnp.zeros_like(pulls)
    x_row[:rows, :] = pos_ref[...]
    x_col[:rows, :] = pos_ref[...]
    x_col[rows:rows + TILE_J, :] = jnp.zeros((TILE_J, width), x_col.dtype)
    spread(meta, h_rows, c_rows, 0)
    append(meta, cols, 0, 0, rows)
    cols[:, cols.shape[1] - TILE_J:] = jnp.zeros((2, TILE_J), jnp.float32)


def state_shapes(rows, width, null, dtype):
    tall = 2 * rows + TILE_I
    return [pltpu.VMEM((tall, width), dtype), pltpu.VMEM((tall, LANES), jnp.float32), pltpu.VMEM((tall, LANES), jnp.float32),
            pltpu.VMEM((null, width), dtype), pltpu.VMEM((2, null + TILE_J), jnp.float32), pltpu.VMEM((width + 8, tall), jnp.float32),
            pltpu.VMEM((tall, LANES), jnp.float32)]


def begin(positions, charges, counts, null):
    rows, width = positions.shape
    groups = rows // LANES
    outs = pl.pallas_call(
        functools.partial(begin_kernel, math.log2(math.e) * 0.5 / width),
        out_shape=[jax.ShapeDtypeStruct((3, groups, LANES), jnp.float32)] + state_shapes(rows, width, null, positions.dtype),
        in_specs=[VMEM_SPEC, VMEM_SPEC, pl.BlockSpec(memory_space=pltpu.SMEM)],
        out_specs=[VMEM_SPEC] * 8,
        compiler_params=pltpu.CompilerParams(vmem_limit_bytes=4 << 20),
        cost_estimate=pl.CostEstimate(flops=1 << 30, bytes_accessed=1 << 20, transcendentals=0),
        name='begin',
    )(positions, charges.reshape(groups, LANES), counts)
    return outs[0], list(outs[1:])


def pair_kernel(cfg, *refs):
    rows, width, scale, this = cfg['rows'], cfg['width'], cfg['scale'], cfg['stage']
    refs = list(refs)
    metas = {k: refs.pop(0) for k in cfg['names']}
    loads = [refs.pop(0) for _ in range(cfg['loads'])]
    mate_pos = refs.pop(0) if this == 0 else None
    incoming = refs.pop(0) if this == cfg['turn'] else None
    n_state = 8 if this > cfg['turn'] else 7
    del refs[:n_state]
    x_row, h_rows, c_rows, x_col, cols, pulls, sums = refs[:7]
    turned = refs[7] if this >= cfg['turn'] else None
    gram_a, gram_b = refs[-2:]
    extra = refs[8 if this >= cfg['turn'] else 7:-2]

    count = {k: jnp.max(metas[k][2, 0:1, :]).astype(jnp.int32) for k in cfg['names']}
    tiles_own = pl.cdiv(count['own'], TILE_I)
    row_mate = pl.multiple_of(up(count['own'], LANES), LANES)
    tiles_both = pl.cdiv(row_mate + count['mate'], TILE_I)

    end = jnp.int32(0)
    lo = jnp.int32(0)
    for stage, chunks in enumerate(cfg['plan'][:this + 1]):
        for k, (name, start, size) in enumerate(chunks):
            if 0 < stage == this:
                at = pl.multiple_of(end, LANES)
                x_col[pl.ds(at, size), :] = loads[k][...]
                x_col[pl.ds(pl.multiple_of(at + size, LANES), TILE_J), :] = jnp.zeros((TILE_J, width), x_col.dtype)
                append(metas[name], cols, at, start, size)
            end = end + up(jnp.clip(count[name] - start, 0, size), LANES)
        tiles = tiles_own if cfg['modes'][stage] == 'own' else tiles_both
        have = pl.cdiv(end, TILE_J) if cfg['close'][stage] else end // TILE_J
        budget = cfg['budget'][stage]
        hi = have if budget is None else jnp.minimum(have, lo + budget // jnp.maximum(tiles, 1))
        if stage < this:
            lo = hi
        if cfg['close'][stage]:
            end = up(end, TILE_J)
    units = (hi - lo) * tiles

    if this == 0:
        x_row[pl.ds(row_mate, rows), :] = mate_pos[...]
        spread(metas['mate'], h_rows, c_rows, row_mate)
    if incoming is not None:
        table = jnp.zeros((LANES, LANES), jnp.float32)
        sub = lax.broadcasted_iota(jnp.int32, (LANES, LANES), 0)
        for g in range(rows // LANES):
            table = jnp.where(sub == g, incoming[width:width + 1, g * LANES:(g + 1) * LANES], table)
        table = table.T
        lane = lax.broadcasted_iota(jnp.int32, (LANES, LANES), 1)
        for g in range(rows // LANES):
            at = slice(g * LANES, (g + 1) * LANES)
            sums[at, :] += jnp.where(lane == 0, table[:, g:g + 1], 0.0)
            for k in range(width // LANES):
                d = slice(k * LANES, (k + 1) * LANES)
                turned[at, d] = (pulls[d, at] + incoming[d, at]).T

    def decode(unit):
        at = jnp.minimum(unit, units - 1)
        j = at // tiles
        return (at - j * tiles) * TILE_I, (j + lo) * TILE_J, jnp.where(unit < units, (j + lo) * TILE_J, cfg['null'])

    def aligned(pos):
        row, col, meta = pos
        return (pl.ds(pl.multiple_of(row, TILE_I), TILE_I), pl.ds(pl.multiple_of(col, TILE_J), TILE_J), pl.multiple_of(meta, TILE_J))

    def gram(pos, out):
        row, col, _ = aligned(pos)
        out[...] = lax.dot_general(x_row[row, :], x_col[col, :], (((1,), (1,)), ((), ())), preferred_element_type=jnp.float32)

    def weigh(pos, prod):
        row, col, meta = aligned(pos)
        h_row, c_row = h_rows[row, :], c_rows[row, :]
        parts, total = [], None
        for k in range(TILE_J // LANES):
            at = pl.ds(pl.multiple_of(meta + k * LANES, LANES), LANES)
            arg = jnp.minimum(prod[:, k * LANES:(k + 1) * LANES] * (2.0 * scale) - h_row - cols[1:2, at], 0.0)
            w = jnp.exp2(arg) * c_row * cols[0:1, at]
            if this == 0:
                off = pos[1] + k * LANES
                off = jnp.where(off < row_mate, off - pos[0], 1 << 20)
                w = jnp.where(lax.broadcasted_iota(jnp.int32, (TILE_I, LANES), 0) - lax.broadcasted_iota(jnp.int32, (TILE_I, LANES), 1) == off, 0.0, w)
            total = w if total is None else total + w
            parts.append(w.astype(jnp.bfloat16))
        sums[row, :] += total
        low = jnp.concatenate(parts, axis=1)
        if turned is None:
            pulls[:width, row] += lax.dot_general(x_col[col, :], low, (((0,), (1,)), ((), ())), preferred_element_type=jnp.float32)
        else:
            turned[row, :] += jnp.dot(low, x_col[col, :], preferred_element_type=jnp.float32)

    @pl.when(units > 0)
    def _():
        first = decode(0)
        gram(first, gram_a)

        def step(p, pos):
            for k in range(UNROLL):
                nxt = decode(UNROLL * p + k + 1)
                gram(nxt, (gram_a, gram_b)[(k + 1) % 2])
                weigh(pos, (gram_a, gram_b)[k % 2])
                pos = nxt
            return pos

        lax.fori_loop(0, pl.cdiv(units, UNROLL), step, first)

    if this == cfg['split']:
        lane = lax.broadcasted_iota(jnp.int32, (LANES, LANES), 1)
        table = jnp.zeros((LANES, LANES), jnp.float32)
        for g in range(rows // LANES):
            at = pl.ds(pl.multiple_of(row_mate + g * LANES, LANES), LANES)
            table = jnp.where(lane == g, jnp.sum(sums[at, :], axis=1, keepdims=True), table)
        table = table.T
        extra[0][:width, :] = pulls[:width, pl.ds(row_mate, rows)]
        for g in range(rows // LANES):
            extra[0][width:, g * LANES:(g + 1) * LANES] = jnp.broadcast_to(table[g:g + 1, :], (8, LANES))
    if this == len(cfg['plan']) - 1:
        force, part = extra
        part[...] = jnp.zeros_like(part)

        def tile(i, carry):
            at = pl.ds(pl.multiple_of(i * LANES, LANES), LANES)
            live = lax.broadcasted_iota(jnp.int32, (LANES, LANES), 0) + i * LANES < count['own']
            lanes = jnp.where(live, sums[at, :], 0.0)
            total = jnp.sum(lanes, axis=1, keepdims=True)
            for k in range(width // LANES):
                d = pl.ds(k * LANES, LANES)
                value = total * x_row[at, d].astype(jnp.float32) - turned[at, d]
                force[at, d] = jnp.where(live, value * cfg['inv_len2'], 0.0)
            part[...] += jnp.sum(lanes.reshape(LANES // 8, 8, LANES), axis=0)
            return carry

        lax.fori_loop(0, rows // LANES, tile, 0, unroll=4)


def pair_call(cfg, stage, metas, chunks, state, mate_pos=None, incoming=None):
    rows, width = cfg['rows'], cfg['width']
    names = ['own', 'mate']
    for chunk in cfg['plan'][:stage + 1]:
        names += [c[0] for c in chunk if c[0] not in names]
    final = stage == len(cfg['plan']) - 1
    cfg = dict(cfg, stage=stage, names=names, loads=len(chunks) if stage else 0)
    args = [metas[k] for k in names] + (list(chunks) if stage else [mate_pos])
    if incoming is not None:
        args.append(incoming)
    aliases = {}
    for k, a in enumerate(state):
        aliases[len(args)] = k
        args.append(a)
    out_shape = state_shapes(rows, width, cfg['null'], jnp.bfloat16)
    if stage >= cfg['turn']:
        out_shape.append(pltpu.VMEM((rows, width), jnp.float32))
    n_state = len(out_shape)
    if stage == cfg['split']:
        out_shape.append(jax.ShapeDtypeStruct((width + 8, rows), jnp.float32))
    if final:
        out_shape += [jax.ShapeDtypeStruct((rows, width), jnp.float32), jax.ShapeDtypeStruct((8, LANES), jnp.float32)]
    outs = pl.pallas_call(
        functools.partial(pair_kernel, cfg),
        out_shape=out_shape,
        in_specs=[VMEM_SPEC] * len(args),
        out_specs=[VMEM_SPEC] * len(out_shape),
        input_output_aliases=aliases,
        scratch_shapes=[pltpu.VMEM((TILE_I, TILE_J), jnp.float32)] * 2,
        compiler_params=pltpu.CompilerParams(vmem_limit_bytes=VMEM_MB[stage] << 20),
        cost_estimate=pl.CostEstimate(flops=1 << 30, bytes_accessed=1 << 20, transcendentals=0),
    )(*args)
    return list(outs[:n_state]), outs[n_state:]


def solution(mesh):
    n = mesh.shape['row']
    forth = [(p, (p + 2) % n if p % 2 == 0 else (p - 2) % n) for p in range(n)]
    back = [(b, a) for a, b in forth]
    twice = [(p, (p + n // 2) % n) for p in range(n)]
    swap = [(p, p ^ 1) for p in range(n)]

    def move(x, perm):
        return lax.ppermute(x, 'row', perm)

    def body(positions, charges, counts):
        block_rows, width = positions.shape
        half_rows = block_rows // 2

        def upper(name):
            return name, 0, half_rows

        def lower(name):
            return name, half_rows, block_rows - half_rows

        plan = [[('own', 0, block_rows)], [upper('near'), upper('next')], [lower('near'), lower('next')],
                [upper('far')], [upper('away')], [lower('far')], [lower('away')]]
        null = up(sum(c[2] for stage in plan for c in stage), TILE_J) + 8 * TILE_J
        cfg = dict(rows=block_rows, width=width, null=null, plan=plan, modes=['both'] * 3 + ['own'] * 4,
                   close=[True, False, True, False, False, False, True], budget=[None, BUDGET, None, None, None, None, None],
                   split=2, turn=4, scale=math.log2(math.e) * 0.5 / width, inv_len2=1.0 / width)

        mate_pos = move(positions, swap)
        top, bottom = positions[:half_rows], positions[half_rows:]
        meta, state = begin(positions, charges, counts, null)
        near_a, next_a = move(top, forth), move(top, back)
        near_b, next_b = move(bottom, forth), move(bottom, back)
        far_a, far_b = move(near_a, forth), move(near_b, forth)
        away_a, away_b = move(far_a, swap), move(far_b, swap)
        far_meta = move(meta, twice)
        metas = {'own': meta, 'mate': move(meta, swap), 'near': move(meta, forth), 'next': move(meta, back),
                 'far': far_meta, 'away': move(far_meta, swap)}
        arrays = [[positions], [near_a, next_a], [near_b, next_b], [far_a], [away_a], [far_b], [away_b]]
        incoming = None
        for stage in range(len(plan)):
            state, out = pair_call(cfg, stage, metas, arrays[stage], state, mate_pos=mate_pos if stage == 0 else None,
                                   incoming=incoming if stage == cfg['turn'] else None)
            if stage == cfg['split']:
                incoming = move(out[0], swap)
        forces, part = out
        return forces, total_energy(part, n)

    row_spec = P(('sys', 'row'), None)
    vec_spec = P(('sys', 'row'))
    step = jax.shard_map(body, mesh=mesh, in_specs=(row_spec, vec_spec, vec_spec), out_specs=(row_spec, P('sys')), check_vma=False)

    def program(positions, charges, counts):
        jax.eval_shape(step, positions, charges, counts)
        return step(positions, charges, counts)

    return program
```

```python
import functools
import math

import jax
import jax.numpy as jnp
from jax import lax
from jax.experimental import pallas as pl
from jax.experimental.pallas import tpu as pltpu
from jax.sharding import PartitionSpec as P


LANES = 128
TILE_I = 256
TILE_J = 512
UNROLL = 4
FIRST_BUDGET = 22
BUDGET = 38
VMEM_MB = (5, 4, 6, 9, 5, 5, 8, 5, 9)
MESH = pl.DeviceIdType.MESH
VMEM_SPEC = pl.BlockSpec(memory_space=pltpu.VMEM)


def energy_kernel(n, part_hbm, out_ref, seen, part_ref, send_sem, recv_sem, local_sem):
    me = lax.axis_index('row')
    barrier = pltpu.get_barrier_semaphore()
    for off in range(1, n):
        pl.semaphore_signal(barrier, inc=1, device_id={'row': lax.rem(me + off, n)}, device_id_type=MESH)
    load = pltpu.make_async_copy(part_hbm, part_ref, local_sem)
    load.start()
    load.wait()
    pl.semaphore_wait(barrier, n - 1)
    copies = []
    for off in range(1, n):
        copies.append(pltpu.make_async_remote_copy(
            src_ref=part_ref, dst_ref=seen.at[me], send_sem=send_sem.at[off - 1], recv_sem=recv_sem.at[off - 1],
            device_id={'row': lax.rem(me + off, n)}, device_id_type=MESH))
    for copy in copies:
        copy.start()
    for copy in copies:
        copy.wait()
    total = jnp.zeros(part_ref.shape, jnp.float32)
    for k in range(n):
        total += jnp.where(me == k, part_ref[...], seen[k])
    out_ref[0] = 0.5 * jnp.sum(total)


def total_energy(part, n):
    return pl.pallas_call(
        functools.partial(energy_kernel, n),
        out_shape=jax.ShapeDtypeStruct((1,), jnp.float32),
        in_specs=[pl.BlockSpec(memory_space=pltpu.HBM)],
        out_specs=pl.BlockSpec(memory_space=pltpu.SMEM),
        scratch_shapes=[pltpu.VMEM((n,) + part.shape, jnp.float32), pltpu.VMEM(part.shape, jnp.float32), pltpu.SemaphoreType.DMA((n - 1,)),
                        pltpu.SemaphoreType.DMA((n - 1,)), pltpu.SemaphoreType.DMA],
        compiler_params=pltpu.CompilerParams(collective_id=0, has_side_effects=True),
        name='energy',
    )(part)


def up(value, step):
    return pl.cdiv(value, step) * step


def spread(meta, h_rows, c_rows, row0):
    groups = meta.shape[1]
    table = jnp.concatenate([meta[0], meta[1], jnp.zeros((LANES - 2 * groups, LANES), jnp.float32)], axis=0).T
    for g in range(groups):
        at = pl.ds(pl.multiple_of(row0 + g * LANES, LANES), LANES)
        c_rows[at, :] = jnp.broadcast_to(table[:, g:g + 1], (LANES, LANES))
        h_rows[at, :] = jnp.broadcast_to(table[:, groups + g:groups + g + 1], (LANES, LANES))


def append(meta, cols, at, start, size):
    for g in range(size // LANES):
        for m in range(2):
            cols[m:m + 1, pl.ds(pl.multiple_of(at + g * LANES, LANES), LANES)] = meta[m, start // LANES + g:start // LANES + g + 1, :]
    cols[:, pl.ds(pl.multiple_of(at + size, LANES), TILE_J)] = jnp.zeros((2, TILE_J), jnp.float32)


def begin_kernel(scale, pos_ref, q_ref, count_ref, meta, x_row, h_rows, c_rows, x_col, cols, pulls, sums):
    rows, width = pos_ref.shape
    lane = lax.broadcasted_iota(jnp.int32, (LANES, LANES), 1)
    table = jnp.zeros((LANES, LANES), jnp.float32)
    for b in range(rows // LANES):
        x = pos_ref[b * LANES:(b + 1) * LANES, :].astype(jnp.float32)
        table = jnp.where(lane == b, jnp.sum(x * x, axis=1, keepdims=True), table)
        meta[0, b:b + 1, :] = jnp.where(lane[:1] + b * LANES < count_ref[0], q_ref[b:b + 1, :], 0.0)
    meta[1] = table.T[:rows // LANES, :] * scale
    meta[2] = jnp.full(meta.shape[1:], count_ref[0], jnp.int32).astype(jnp.float32)
    sums[...] = jnp.zeros_like(sums)
    pulls[...] = jnp.zeros_like(pulls)
    x_row[:rows, :] = pos_ref[...]
    x_col[:rows, :] = pos_ref[...]
    x_col[rows:rows + TILE_J, :] = jnp.zeros((TILE_J, width), x_col.dtype)
    spread(meta, h_rows, c_rows, 0)
    append(meta, cols, 0, 0, rows)
    cols[:, cols.shape[1] - TILE_J:] = jnp.zeros((2, TILE_J), jnp.float32)


def state_shapes(rows, width, null, dtype):
    tall = 2 * rows + TILE_I
    return [pltpu.VMEM((tall, width), dtype), pltpu.VMEM((tall, LANES), jnp.float32), pltpu.VMEM((tall, LANES), jnp.float32),
            pltpu.VMEM((null, width), dtype), pltpu.VMEM((2, null + TILE_J), jnp.float32), pltpu.VMEM((width + 8, tall), jnp.float32),
            pltpu.VMEM((tall, LANES), jnp.float32)]


def begin(positions, charges, counts, null):
    rows, width = positions.shape
    groups = rows // LANES
    outs = pl.pallas_call(
        functools.partial(begin_kernel, math.log2(math.e) * 0.5 / width),
        out_shape=[jax.ShapeDtypeStruct((3, groups, LANES), jnp.float32)] + state_shapes(rows, width, null, positions.dtype),
        in_specs=[VMEM_SPEC, VMEM_SPEC, pl.BlockSpec(memory_space=pltpu.SMEM)],
        out_specs=[VMEM_SPEC] * 8,
        compiler_params=pltpu.CompilerParams(vmem_limit_bytes=4 << 20),
        cost_estimate=pl.CostEstimate(flops=1 << 30, bytes_accessed=1 << 20, transcendentals=0),
        name='begin',
    )(positions, charges.reshape(groups, LANES), counts)
    return outs[0], list(outs[1:])


def pair_kernel(cfg, *refs):
    rows, width, scale, this = cfg['rows'], cfg['width'], cfg['scale'], cfg['stage']
    refs = list(refs)
    metas = {k: refs.pop(0) for k in cfg['names']}
    loads = [refs.pop(0) for _ in range(cfg['loads'])]
    mate_pos = refs.pop(0) if this == 0 else None
    incoming = refs.pop(0) if this == cfg['turn'] else None
    n_state = 8 if this > cfg['turn'] else 7
    del refs[:n_state]
    x_row, h_rows, c_rows, x_col, cols, pulls, sums = refs[:7]
    turned = refs[7] if this >= cfg['turn'] else None
    refs = refs[8 if this >= cfg['turn'] else 7:]
    n_out = (this == cfg['split']) + 2 * (this == len(cfg['plan']) - 1)
    gram_a, gram_b = refs[n_out:n_out + 2]
    extra = refs[:n_out] + refs[n_out + 2:]

    count = {k: jnp.max(metas[k][2, 0:1, :]).astype(jnp.int32) for k in cfg['names']}
    tiles_own = pl.cdiv(count['own'], TILE_I)
    row_mate = pl.multiple_of(up(count['own'], LANES), LANES)
    tiles_both = pl.cdiv(row_mate + count['mate'], TILE_I)

    end = jnp.int32(0)
    lo = jnp.int32(0)
    for stage, chunks in enumerate(cfg['plan'][:this + 1]):
        for k, (name, start, size) in enumerate(chunks):
            if 0 < stage == this:
                at = pl.multiple_of(end, LANES)
                x_col[pl.ds(at, size), :] = loads[k][...]
                x_col[pl.ds(pl.multiple_of(at + size, LANES), TILE_J), :] = jnp.zeros((TILE_J, width), x_col.dtype)
                append(metas[name], cols, at, start, size)
            end = end + up(jnp.clip(count[name] - start, 0, size), LANES)
        tiles = tiles_own if cfg['modes'][stage] == 'own' else tiles_both
        have = pl.cdiv(end, TILE_J) if cfg['close'][stage] else end // TILE_J
        budget = cfg['budget'][stage]
        hi = have if budget is None else jnp.minimum(have, lo + budget // jnp.maximum(tiles, 1))
        if stage < this:
            lo = hi
        if cfg['close'][stage]:
            end = up(end, TILE_J)
    units = (hi - lo) * tiles

    if this == 0:
        x_row[pl.ds(row_mate, rows), :] = mate_pos[...]
        spread(metas['mate'], h_rows, c_rows, row_mate)
    if incoming is not None:
        table = jnp.zeros((LANES, LANES), jnp.float32)
        sub = lax.broadcasted_iota(jnp.int32, (LANES, LANES), 0)
        for g in range(rows // LANES):
            table = jnp.where(sub == g, incoming[width:width + 1, g * LANES:(g + 1) * LANES], table)
        table = table.T
        lane = lax.broadcasted_iota(jnp.int32, (LANES, LANES), 1)
        for g in range(rows // LANES):
            at = slice(g * LANES, (g + 1) * LANES)
            sums[at, :] += jnp.where(lane == 0, table[:, g:g + 1], 0.0)
            for k in range(width // LANES):
                d = slice(k * LANES, (k + 1) * LANES)
                turned[at, d] = (pulls[d, at] + incoming[d, at]).T

    def decode(unit):
        at = jnp.minimum(unit, units - 1)
        j = at // tiles
        return (at - j * tiles) * TILE_I, (j + lo) * TILE_J

    def aligned(pos):
        return pl.ds(pl.multiple_of(pos[0], TILE_I), TILE_I), pl.ds(pl.multiple_of(pos[1], TILE_J), TILE_J)

    def gram(pos, out):
        row, col = aligned(pos)
        out[...] = lax.dot_general(x_row[row, :], x_col[col, :], (((1,), (1,)), ((), ())), preferred_element_type=jnp.float32)

    def weigh(pos, prod):
        row, col = aligned(pos)
        h_row, c_row = h_rows[row, :], c_rows[row, :]
        parts, total = [], None
        for k in range(TILE_J // LANES):
            at = pl.ds(pl.multiple_of(pos[1] + k * LANES, LANES), LANES)
            arg = jnp.minimum(prod[:, k * LANES:(k + 1) * LANES] * (2.0 * scale) - h_row - cols[1:2, at], 0.0)
            w = jnp.exp2(arg) * c_row * cols[0:1, at]
            if this < 2:
                off = pos[1] + k * LANES
                off = jnp.where(off < row_mate, off - pos[0], 1 << 20)
                w = jnp.where(lax.broadcasted_iota(jnp.int32, (TILE_I, LANES), 0) - lax.broadcasted_iota(jnp.int32, (TILE_I, LANES), 1) == off, 0.0, w)
            total = w if total is None else total + w
            parts.append(w.astype(jnp.bfloat16))
        sums[row, :] += total
        low = jnp.concatenate(parts, axis=1)
        if turned is None:
            pulls[:width, row] += lax.dot_general(x_col[col, :], low, (((0,), (1,)), ((), ())), preferred_element_type=jnp.float32)
        else:
            turned[row, :] += jnp.dot(low, x_col[col, :], preferred_element_type=jnp.float32)

    @pl.when((units > 0) if cfg['plan'][this] or this < 2 else False)
    def _():
        first = decode(0)
        gram(first, gram_a)

        def step(p, pos):
            for k in range(UNROLL):
                nxt = decode(UNROLL * p + k + 1)
                gram(nxt, (gram_a, gram_b)[(k + 1) % 2])
                weigh(pos, (gram_a, gram_b)[k % 2])
                pos = nxt
            return pos

        def single(unit, pos):
            nxt = decode(unit + 1)
            weigh(pos, gram_a)
            gram(nxt, gram_a)
            return nxt

        whole = units // UNROLL
        lax.fori_loop(whole * UNROLL, units, single, lax.fori_loop(0, whole, step, first))

    if this == cfg['split']:
        lane = lax.broadcasted_iota(jnp.int32, (LANES, LANES), 1)
        table = jnp.zeros((LANES, LANES), jnp.float32)
        for g in range(rows // LANES):
            at = pl.ds(pl.multiple_of(row_mate + g * LANES, LANES), LANES)
            table = jnp.where(lane == g, jnp.sum(sums[at, :], axis=1, keepdims=True), table)
        table = table.T
        extra[0][:width, :] = pulls[:width, pl.ds(row_mate, rows)]
        for g in range(rows // LANES):
            extra[0][width:, g * LANES:(g + 1) * LANES] = jnp.broadcast_to(table[g:g + 1, :], (8, LANES))
    if this == len(cfg['plan']) - 1:
        force, part = extra[:2]
        staged, copy_sem = extra[2:]
        part[...] = jnp.zeros_like(part)
        step = rows // copy_sem.shape[0]

        def tile(i, carry):
            at = pl.ds(pl.multiple_of(i * LANES, LANES), LANES)
            live = lax.broadcasted_iota(jnp.int32, (LANES, LANES), 0) + i * LANES < count['own']
            lanes = jnp.where(live, sums[at, :], 0.0)
            total = jnp.sum(lanes, axis=1, keepdims=True)
            for k in range(width // LANES):
                d = pl.ds(k * LANES, LANES)
                value = total * x_row[at, d].astype(jnp.float32) - turned[at, d]
                staged[at, d] = jnp.where(live, value * cfg['inv_len2'], 0.0)
            part[...] += jnp.sum(lanes.reshape(LANES // 8, 8, LANES), axis=0)
            return carry

        copies = []
        for q in range(copy_sem.shape[0]):
            lax.fori_loop(q * step // LANES, (q + 1) * step // LANES, tile, 0, unroll=True)
            at = pl.ds(q * step, step)
            copies.append(pltpu.make_async_copy(staged.at[at, :], force.at[at, :], copy_sem.at[q]))
            copies[-1].start()
        for copy in copies:
            copy.wait()


def pair_call(cfg, stage, metas, chunks, state, mate_pos=None, incoming=None):
    rows, width = cfg['rows'], cfg['width']
    names = ['own', 'mate']
    for chunk in cfg['plan'][:stage + 1]:
        names += [c[0] for c in chunk if c[0] not in names]
    final = stage == len(cfg['plan']) - 1
    cfg = dict(cfg, stage=stage, names=names, loads=len(chunks) if stage else 0)
    args = [metas[k] for k in names] + (list(chunks) if stage else [mate_pos])
    if incoming is not None:
        args.append(incoming)
    aliases = {}
    for k, a in enumerate(state):
        aliases[len(args)] = k
        args.append(a)
    out_shape = state_shapes(rows, width, cfg['null'], jnp.bfloat16)
    if stage >= cfg['turn']:
        out_shape.append(pltpu.VMEM((rows, width), jnp.float32))
    n_state = len(out_shape)
    if stage == cfg['split']:
        out_shape.append(jax.ShapeDtypeStruct((width + 8, rows), jnp.float32))
    if final:
        out_shape += [jax.ShapeDtypeStruct((rows, width), jnp.float32), jax.ShapeDtypeStruct((8, LANES), jnp.float32)]
    out_specs = [VMEM_SPEC] * len(out_shape)
    scratch = []
    if final:
        out_specs[n_state] = pl.BlockSpec(memory_space=pltpu.HBM)
        scratch = [pltpu.VMEM((rows, width), jnp.float32), pltpu.SemaphoreType.DMA((4,))]
    outs = pl.pallas_call(
        functools.partial(pair_kernel, cfg),
        out_shape=out_shape,
        in_specs=[VMEM_SPEC] * len(args),
        out_specs=out_specs,
        input_output_aliases=aliases,
        scratch_shapes=[pltpu.VMEM((TILE_I, TILE_J), jnp.float32)] * 2 + scratch,
        compiler_params=pltpu.CompilerParams(vmem_limit_bytes=VMEM_MB[stage] << 20),
        cost_estimate=pl.CostEstimate(flops=1 << 30, bytes_accessed=1 << 20, transcendentals=0),
    )(*args)
    return list(outs[:n_state]), outs[n_state:]


def solution(mesh):
    n = mesh.shape['row']
    forth = [(p, (p + 2) % n if p % 2 == 0 else (p - 2) % n) for p in range(n)]
    back = [(b, a) for a, b in forth]
    twice = [(p, (p + n // 2) % n) for p in range(n)]
    swap = [(p, p ^ 1) for p in range(n)]

    def move(x, perm):
        return lax.ppermute(x, 'row', perm)

    def body(positions, charges, counts):
        block_rows, width = positions.shape
        half_rows = block_rows // 2

        def upper(name):
            return name, 0, half_rows

        def lower(name):
            return name, half_rows, block_rows - half_rows

        plan = [[('own', 0, block_rows)], [], [upper('near'), upper('next')], [lower('near'), lower('next')],
                [upper('far')], [upper('away')], [], [lower('far')], [lower('away')]]
        null = up(sum(c[2] for stage in plan for c in stage), TILE_J) + 8 * TILE_J
        cfg = dict(rows=block_rows, width=width, null=null, plan=plan, modes=['both'] * 4 + ['own'] * 5,
                   close=[True, True, False, True, False, False, False, False, True],
                   budget=[FIRST_BUDGET, None, BUDGET] + [None] * 6,
                   split=3, turn=6, scale=math.log2(math.e) * 0.5 / width, inv_len2=1.0 / width)

        mate_pos = move(positions, swap)
        top, bottom = positions[:half_rows], positions[half_rows:]
        meta, state = begin(positions, charges, counts, null)
        near_a, next_a = move(top, forth), move(top, back)
        near_b, next_b = move(bottom, forth), move(bottom, back)
        far_a, far_b = move(near_a, forth), move(near_b, forth)
        away_a, away_b = move(far_a, swap), move(far_b, swap)
        far_meta = move(meta, twice)
        metas = {'own': meta, 'mate': move(meta, swap), 'near': move(meta, forth), 'next': move(meta, back),
                 'far': far_meta, 'away': move(far_meta, swap)}
        arrays = [[positions], [], [near_a, next_a], [near_b, next_b], [far_a], [away_a], [], [far_b], [away_b]]
        incoming = None
        for stage in range(len(plan)):
            state, out = pair_call(cfg, stage, metas, arrays[stage], state, mate_pos=mate_pos if stage == 0 else None,
                                   incoming=incoming if stage == cfg['turn'] else None)
            if stage == cfg['split']:
                incoming = move(out[0], swap)
        forces, part = out
        return forces, total_energy(part, n)

    row_spec = P(('sys', 'row'), None)
    vec_spec = P(('sys', 'row'))
    step = jax.shard_map(body, mesh=mesh, in_specs=(row_spec, vec_spec, vec_spec), out_specs=(row_spec, P('sys')), check_vma=False)

    def program(positions, charges, counts):
        jax.eval_shape(step, positions, charges, counts)
        return step(positions, charges, counts)

    return program
```

```python
import functools
import math

import jax
import jax.numpy as jnp
from jax import lax
from jax.experimental import pallas as pl
from jax.experimental.pallas import tpu as pltpu
from jax.sharding import PartitionSpec as P


LANES = 128
TILE_I = 256
TILE_J = 512
UNROLL = 4
BUDGET = 74
VMEM_MB = (5, 6, 9, 5, 5, 8, 5, 9)
MESH = pl.DeviceIdType.MESH
VMEM_SPEC = pl.BlockSpec(memory_space=pltpu.VMEM)


def energy_kernel(n, part_hbm, out_ref, seen, part_ref, send_sem, recv_sem, local_sem):
    me = lax.axis_index('row')
    barrier = pltpu.get_barrier_semaphore()
    for off in range(1, n):
        pl.semaphore_signal(barrier, inc=1, device_id={'row': lax.rem(me + off, n)}, device_id_type=MESH)
    load = pltpu.make_async_copy(part_hbm, part_ref, local_sem)
    load.start()
    load.wait()
    pl.semaphore_wait(barrier, n - 1)
    copies = []
    for off in range(1, n):
        copies.append(pltpu.make_async_remote_copy(
            src_ref=part_ref, dst_ref=seen.at[me], send_sem=send_sem.at[off - 1], recv_sem=recv_sem.at[off - 1],
            device_id={'row': lax.rem(me + off, n)}, device_id_type=MESH))
    for copy in copies:
        copy.start()
    for copy in copies:
        copy.wait()
    total = jnp.zeros(part_ref.shape, jnp.float32)
    for k in range(n):
        total += jnp.where(me == k, part_ref[...], seen[k])
    out_ref[0] = 0.5 * jnp.sum(total)


def total_energy(part, n):
    return pl.pallas_call(
        functools.partial(energy_kernel, n),
        out_shape=jax.ShapeDtypeStruct((1,), jnp.float32),
        in_specs=[pl.BlockSpec(memory_space=pltpu.HBM)],
        out_specs=pl.BlockSpec(memory_space=pltpu.SMEM),
        scratch_shapes=[pltpu.VMEM((n,) + part.shape, jnp.float32), pltpu.VMEM(part.shape, jnp.float32), pltpu.SemaphoreType.DMA((n - 1,)),
                        pltpu.SemaphoreType.DMA((n - 1,)), pltpu.SemaphoreType.DMA],
        compiler_params=pltpu.CompilerParams(collective_id=0, has_side_effects=True),
        name='energy',
    )(part)


def up(value, step):
    return pl.cdiv(value, step) * step


def spread(meta, h_rows, c_rows, row0):
    groups = meta.shape[1]
    table = jnp.concatenate([meta[0], meta[1], jnp.zeros((LANES - 2 * groups, LANES), jnp.float32)], axis=0).T
    for g in range(groups):
        at = pl.ds(pl.multiple_of(row0 + g * LANES, LANES), LANES)
        c_rows[at, :] = jnp.broadcast_to(table[:, g:g + 1], (LANES, LANES))
        h_rows[at, :] = jnp.broadcast_to(table[:, groups + g:groups + g + 1], (LANES, LANES))


def append(meta, cols, at, start, size):
    for g in range(size // LANES):
        for m in range(2):
            cols[m:m + 1, pl.ds(pl.multiple_of(at + g * LANES, LANES), LANES)] = meta[m, start // LANES + g:start // LANES + g + 1, :]
    cols[:, pl.ds(pl.multiple_of(at + size, LANES), TILE_J)] = jnp.zeros((2, TILE_J), jnp.float32)


def begin_kernel(scale, pos_ref, q_ref, count_ref, meta, x_row, h_rows, c_rows, x_col, cols, pulls, sums):
    rows, width = pos_ref.shape
    lane = lax.broadcasted_iota(jnp.int32, (LANES, LANES), 1)
    table = jnp.zeros((LANES, LANES), jnp.float32)
    for b in range(rows // LANES):
        x = pos_ref[b * LANES:(b + 1) * LANES, :].astype(jnp.float32)
        table = jnp.where(lane == b, jnp.sum(x * x, axis=1, keepdims=True), table)
        meta[0, b:b + 1, :] = jnp.where(lane[:1] + b * LANES < count_ref[0], q_ref[b:b + 1, :], 0.0)
    meta[1] = table.T[:rows // LANES, :] * scale
    meta[2] = jnp.full(meta.shape[1:], count_ref[0], jnp.int32).astype(jnp.float32)
    sums[...] = jnp.zeros_like(sums)
    pulls[...] = jnp.zeros_like(pulls)
    x_row[:rows, :] = pos_ref[...]
    x_col[:rows, :] = pos_ref[...]
    x_col[rows:rows + TILE_J, :] = jnp.zeros((TILE_J, width), x_col.dtype)
    spread(meta, h_rows, c_rows, 0)
    append(meta, cols, 0, 0, rows)
    cols[:, cols.shape[1] - TILE_J:] = jnp.zeros((2, TILE_J), jnp.float32)


def state_shapes(rows, width, null, dtype):
    tall = 2 * rows + TILE_I
    return [pltpu.VMEM((tall, width), dtype), pltpu.VMEM((tall, LANES), jnp.float32), pltpu.VMEM((tall, LANES), jnp.float32),
            pltpu.VMEM((null, width), dtype), pltpu.VMEM((2, null + TILE_J), jnp.float32), pltpu.VMEM((width + 8, tall), jnp.float32),
            pltpu.VMEM((tall, LANES), jnp.float32)]


def begin(positions, charges, counts, null):
    rows, width = positions.shape
    groups = rows // LANES
    outs = pl.pallas_call(
        functools.partial(begin_kernel, math.log2(math.e) * 0.5 / width),
        out_shape=[jax.ShapeDtypeStruct((3, groups, LANES), jnp.float32)] + state_shapes(rows, width, null, positions.dtype),
        in_specs=[VMEM_SPEC, VMEM_SPEC, pl.BlockSpec(memory_space=pltpu.SMEM)],
        out_specs=[VMEM_SPEC] * 8,
        compiler_params=pltpu.CompilerParams(vmem_limit_bytes=4 << 20),
        cost_estimate=pl.CostEstimate(flops=1 << 30, bytes_accessed=1 << 20, transcendentals=0),
        name='begin',
    )(positions, charges.reshape(groups, LANES), counts)
    return outs[0], list(outs[1:])


def pair_kernel(cfg, *refs):
    rows, width, scale, this = cfg['rows'], cfg['width'], cfg['scale'], cfg['stage']
    refs = list(refs)
    metas = {k: refs.pop(0) for k in cfg['names']}
    loads = [refs.pop(0) for _ in range(cfg['loads'])]
    mate_pos = refs.pop(0) if this == 0 else None
    incoming = refs.pop(0) if this == cfg['turn'] else None
    n_state = 8 if this > cfg['turn'] else 7
    del refs[:n_state]
    x_row, h_rows, c_rows, x_col, cols, pulls, sums = refs[:7]
    turned = refs[7] if this >= cfg['turn'] else None
    refs = refs[8 if this >= cfg['turn'] else 7:]
    n_out = (this == cfg['split']) + 2 * (this == len(cfg['plan']) - 1)
    gram_a, gram_b = refs[n_out:n_out + 2]
    extra = refs[:n_out] + refs[n_out + 2:]

    count = {k: jnp.max(metas[k][2, 0:1, :]).astype(jnp.int32) for k in cfg['names']}
    tiles_own = pl.cdiv(count['own'], TILE_I)
    row_mate = pl.multiple_of(up(count['own'], LANES), LANES)
    tiles_both = pl.cdiv(row_mate + count['mate'], TILE_I)

    end = jnp.int32(0)
    lo = jnp.int32(0)
    for stage, chunks in enumerate(cfg['plan'][:this + 1]):
        for k, (name, start, size) in enumerate(chunks):
            if 0 < stage == this:
                at = pl.multiple_of(end, LANES)
                x_col[pl.ds(at, size), :] = loads[k][...]
                x_col[pl.ds(pl.multiple_of(at + size, LANES), TILE_J), :] = jnp.zeros((TILE_J, width), x_col.dtype)
                append(metas[name], cols, at, start, size)
            end = end + up(jnp.clip(count[name] - start, 0, size), LANES)
        tiles = tiles_own if cfg['modes'][stage] == 'own' else tiles_both
        have = pl.cdiv(end, TILE_J) if cfg['close'][stage] else end // TILE_J
        budget = cfg['budget'][stage]
        hi = have if budget is None else jnp.minimum(have, jnp.maximum(lo, budget // jnp.maximum(tiles, 1)))
        if stage < this:
            lo = hi
        if cfg['close'][stage]:
            end = up(end, TILE_J)
    if this == 0:
        x_row[pl.ds(row_mate, rows), :] = mate_pos[...]
        spread(metas['mate'], h_rows, c_rows, row_mate)
    if incoming is not None:
        table = jnp.zeros((LANES, LANES), jnp.float32)
        sub = lax.broadcasted_iota(jnp.int32, (LANES, LANES), 0)
        for g in range(rows // LANES):
            table = jnp.where(sub == g, incoming[width:width + 1, g * LANES:(g + 1) * LANES], table)
        table = table.T
        lane = lax.broadcasted_iota(jnp.int32, (LANES, LANES), 1)
        for g in range(rows // LANES):
            at = slice(g * LANES, (g + 1) * LANES)
            sums[at, :] += jnp.where(lane == 0, table[:, g:g + 1], 0.0)
            for k in range(width // LANES):
                d = slice(k * LANES, (k + 1) * LANES)
                turned[at, d] = (pulls[d, at] + incoming[d, at]).T

    def aligned(pos):
        return pl.ds(pl.multiple_of(pos[0], TILE_I), TILE_I), pl.ds(pl.multiple_of(pos[1], TILE_J), TILE_J)

    def gram(pos, out):
        row, col = aligned(pos)
        out[...] = lax.dot_general(x_row[row, :], x_col[col, :], (((1,), (1,)), ((), ())), preferred_element_type=jnp.float32)

    def weigh(pos, prod, diag):
        row, col = aligned(pos)
        h_row, c_row = h_rows[row, :], c_rows[row, :]
        parts, total = [], None
        for k in range(TILE_J // LANES):
            at = pl.ds(pl.multiple_of(pos[1] + k * LANES, LANES), LANES)
            arg = jnp.minimum(prod[:, k * LANES:(k + 1) * LANES] * (2.0 * scale) - h_row - cols[1:2, at], 0.0)
            w = jnp.exp2(arg) * c_row * cols[0:1, at]
            if diag:
                off = pos[1] + k * LANES
                off = jnp.where(off < row_mate, off - pos[0], 1 << 20)
                w = jnp.where(lax.broadcasted_iota(jnp.int32, (TILE_I, LANES), 0) - lax.broadcasted_iota(jnp.int32, (TILE_I, LANES), 1) == off, 0.0, w)
            total = w if total is None else total + w
            parts.append(w.astype(jnp.bfloat16))
        sums[row, :] += total
        low = jnp.concatenate(parts, axis=1)
        if turned is None:
            pulls[:width, row] += lax.dot_general(x_col[col, :], low, (((0,), (1,)), ((), ())), preferred_element_type=jnp.float32)
        else:
            turned[row, :] += jnp.dot(low, x_col[col, :], preferred_element_type=jnp.float32)

    def run(units, decode, unroll, diag=False):
        @pl.when(units > 0)
        def _():
            first = decode(0)
            gram(first, gram_a)

            def step(p, pos):
                for k in range(unroll):
                    nxt = decode(jnp.minimum(unroll * p + k + 1, units - 1))
                    gram(nxt, (gram_a, gram_b)[(k + 1) % 2])
                    weigh(pos, (gram_a, gram_b)[k % 2], diag)
                    pos = nxt
                return pos

            def single(unit, pos):
                nxt = decode(jnp.minimum(unit + 1, units - 1))
                weigh(pos, gram_a, diag)
                gram(nxt, gram_a)
                return nxt

            whole = units // unroll
            last = lax.fori_loop(0, whole, step, first)
            if not diag:
                lax.fori_loop(whole * unroll, units, single, last)

    if this == 0:
        per_col = TILE_J // TILE_I
        rest = jnp.maximum(tiles - per_col, per_col * hi - per_col)

        def off_diag(unit):
            j = unit // jnp.maximum(rest, 1)
            i = unit - j * rest
            return jnp.where(i < per_col * j, i, i + per_col) * TILE_I, j * TILE_J

        run(per_col * hi, lambda unit: (unit * TILE_I, unit // per_col * TILE_J), per_col, diag=True)
        run(jnp.where(rest > 0, rest * hi, 0), off_diag, UNROLL)
    elif cfg['loads']:
        def plain(unit):
            j = unit // tiles
            return (unit - j * tiles) * TILE_I, (j + lo) * TILE_J

        run((hi - lo) * tiles, plain, UNROLL)

    if this == cfg['split']:
        lane = lax.broadcasted_iota(jnp.int32, (LANES, LANES), 1)
        table = jnp.zeros((LANES, LANES), jnp.float32)
        for g in range(rows // LANES):
            at = pl.ds(pl.multiple_of(row_mate + g * LANES, LANES), LANES)
            table = jnp.where(lane == g, jnp.sum(sums[at, :], axis=1, keepdims=True), table)
        table = table.T
        extra[0][:width, :] = pulls[:width, pl.ds(row_mate, rows)]
        for g in range(rows // LANES):
            extra[0][width:, g * LANES:(g + 1) * LANES] = jnp.broadcast_to(table[g:g + 1, :], (8, LANES))
    if this == len(cfg['plan']) - 1:
        force, part = extra[:2]
        staged, copy_sem = extra[2:]
        part[...] = jnp.zeros_like(part)
        step = rows // copy_sem.shape[0]

        def tile(i, carry):
            at = pl.ds(pl.multiple_of(i * LANES, LANES), LANES)
            live = lax.broadcasted_iota(jnp.int32, (LANES, LANES), 0) + i * LANES < count['own']
            lanes = jnp.where(live, sums[at, :], 0.0)
            total = jnp.sum(lanes, axis=1, keepdims=True)
            for k in range(width // LANES):
                d = pl.ds(k * LANES, LANES)
                value = total * x_row[at, d].astype(jnp.float32) - turned[at, d]
                staged[at, d] = jnp.where(live, value * cfg['inv_len2'], 0.0)
            part[...] += jnp.sum(lanes.reshape(LANES // 8, 8, LANES), axis=0)
            return carry

        copies = []
        for q in range(copy_sem.shape[0]):
            lax.fori_loop(q * step // LANES, (q + 1) * step // LANES, tile, 0, unroll=True)
            at = pl.ds(q * step, step)
            copies.append(pltpu.make_async_copy(staged.at[at, :], force.at[at, :], copy_sem.at[q]))
            copies[-1].start()
        for copy in copies:
            copy.wait()


def pair_call(cfg, stage, metas, chunks, state, mate_pos=None, incoming=None):
    rows, width = cfg['rows'], cfg['width']
    names = ['own', 'mate']
    for chunk in cfg['plan'][:stage + 1]:
        names += [c[0] for c in chunk if c[0] not in names]
    final = stage == len(cfg['plan']) - 1
    cfg = dict(cfg, stage=stage, names=names, loads=len(chunks) if stage else 0)
    args = [metas[k] for k in names] + (list(chunks) if stage else [mate_pos])
    if incoming is not None:
        args.append(incoming)
    aliases = {}
    for k, a in enumerate(state):
        aliases[len(args)] = k
        args.append(a)
    out_shape = state_shapes(rows, width, cfg['null'], jnp.bfloat16)
    if stage >= cfg['turn']:
        out_shape.append(pltpu.VMEM((rows, width), jnp.float32))
    n_state = len(out_shape)
    if stage == cfg['split']:
        out_shape.append(jax.ShapeDtypeStruct((width + 8, rows), jnp.float32))
    if final:
        out_shape += [jax.ShapeDtypeStruct((rows, width), jnp.float32), jax.ShapeDtypeStruct((8, LANES), jnp.float32)]
    out_specs = [VMEM_SPEC] * len(out_shape)
    scratch = []
    if final:
        out_specs[n_state] = pl.BlockSpec(memory_space=pltpu.HBM)
        scratch = [pltpu.VMEM((rows, width), jnp.float32), pltpu.SemaphoreType.DMA((4,))]
    outs = pl.pallas_call(
        functools.partial(pair_kernel, cfg),
        out_shape=out_shape,
        in_specs=[VMEM_SPEC] * len(args),
        out_specs=out_specs,
        input_output_aliases=aliases,
        scratch_shapes=[pltpu.VMEM((TILE_I, TILE_J), jnp.float32)] * 2 + scratch,
        compiler_params=pltpu.CompilerParams(vmem_limit_bytes=VMEM_MB[stage] << 20),
        cost_estimate=pl.CostEstimate(flops=1 << 30, bytes_accessed=1 << 20, transcendentals=0),
    )(*args)
    return list(outs[:n_state]), outs[n_state:]


def solution(mesh):
    n = mesh.shape['row']
    forth = [(p, (p + 2) % n if p % 2 == 0 else (p - 2) % n) for p in range(n)]
    back = [(b, a) for a, b in forth]
    twice = [(p, (p + n // 2) % n) for p in range(n)]
    swap = [(p, p ^ 1) for p in range(n)]

    def move(x, perm):
        return lax.ppermute(x, 'row', perm)

    def body(positions, charges, counts):
        block_rows, width = positions.shape
        half_rows = block_rows // 2

        def upper(name):
            return name, 0, half_rows

        def lower(name):
            return name, half_rows, block_rows - half_rows

        plan = [[('own', 0, block_rows)], [upper('near'), upper('next')], [lower('near'), lower('next')],
                [upper('far')], [upper('away')], [], [lower('far')], [lower('away')]]
        null = up(sum(c[2] for stage in plan for c in stage), TILE_J) + 8 * TILE_J
        cfg = dict(rows=block_rows, width=width, null=null, plan=plan, modes=['both'] * 3 + ['own'] * 5,
                   close=[True, False, True, False, False, False, False, True],
                   budget=[None, BUDGET] + [None] * 6,
                   split=2, turn=5, scale=math.log2(math.e) * 0.5 / width, inv_len2=1.0 / width)

        mate_pos = move(positions, swap)
        top, bottom = positions[:half_rows], positions[half_rows:]
        meta, state = begin(positions, charges, counts, null)
        near_a, next_a = move(top, forth), move(top, back)
        near_b, next_b = move(bottom, forth), move(bottom, back)
        far_a, far_b = move(near_a, forth), move(near_b, forth)
        away_a, away_b = move(far_a, swap), move(far_b, swap)
        far_meta = move(meta, twice)
        metas = {'own': meta, 'mate': move(meta, swap), 'near': move(meta, forth), 'next': move(meta, back),
                 'far': far_meta, 'away': move(far_meta, swap)}
        arrays = [[positions], [near_a, next_a], [near_b, next_b], [far_a], [away_a], [], [far_b], [away_b]]
        incoming = None
        for stage in range(len(plan)):
            state, out = pair_call(cfg, stage, metas, arrays[stage], state, mate_pos=mate_pos if stage == 0 else None,
                                   incoming=incoming if stage == cfg['turn'] else None)
            if stage == cfg['split']:
                incoming = move(out[0], swap)
        forces, part = out
        return forces, total_energy(part, n)

    row_spec = P(('sys', 'row'), None)
    vec_spec = P(('sys', 'row'))
    step = jax.shard_map(body, mesh=mesh, in_specs=(row_spec, vec_spec, vec_spec), out_specs=(row_spec, P('sys')), check_vma=False)

    def program(positions, charges, counts):
        jax.eval_shape(step, positions, charges, counts)
        return step(positions, charges, counts)

    return program
```

```python
import functools
import math

import jax
import jax.numpy as jnp
from jax import lax
from jax.experimental import pallas as pl
from jax.experimental.pallas import tpu as pltpu
from jax.sharding import PartitionSpec as P


LANES = 128
TILE_I = 256
TILE_J = 512
UNROLL = 4
BUDGET = 74
VMEM_MB = (5, 6, 6, 9, 5, 8, 9)
MESH = pl.DeviceIdType.MESH
VMEM_SPEC = pl.BlockSpec(memory_space=pltpu.VMEM)


def energy_kernel(n, part_hbm, out_ref, seen, part_ref, send_sem, recv_sem, local_sem):
    me = lax.axis_index('row')
    barrier = pltpu.get_barrier_semaphore()
    for off in range(1, n):
        pl.semaphore_signal(barrier, inc=1, device_id={'row': lax.rem(me + off, n)}, device_id_type=MESH)
    load = pltpu.make_async_copy(part_hbm, part_ref, local_sem)
    load.start()
    load.wait()
    pl.semaphore_wait(barrier, n - 1)
    copies = []
    for off in range(1, n):
        copies.append(pltpu.make_async_remote_copy(
            src_ref=part_ref, dst_ref=seen.at[me], send_sem=send_sem.at[off - 1], recv_sem=recv_sem.at[off - 1],
            device_id={'row': lax.rem(me + off, n)}, device_id_type=MESH))
    for copy in copies:
        copy.start()
    for copy in copies:
        copy.wait()
    total = jnp.zeros(part_ref.shape, jnp.float32)
    for k in range(n):
        total += jnp.where(me == k, part_ref[...], seen[k])
    out_ref[0] = 0.5 * jnp.sum(total)


def total_energy(part, n):
    return pl.pallas_call(
        functools.partial(energy_kernel, n),
        out_shape=jax.ShapeDtypeStruct((1,), jnp.float32),
        in_specs=[pl.BlockSpec(memory_space=pltpu.HBM)],
        out_specs=pl.BlockSpec(memory_space=pltpu.SMEM),
        scratch_shapes=[pltpu.VMEM((n,) + part.shape, jnp.float32), pltpu.VMEM(part.shape, jnp.float32), pltpu.SemaphoreType.DMA((n - 1,)),
                        pltpu.SemaphoreType.DMA((n - 1,)), pltpu.SemaphoreType.DMA],
        compiler_params=pltpu.CompilerParams(collective_id=0, has_side_effects=True),
        name='energy',
    )(part)


def up(value, step):
    return pl.cdiv(value, step) * step


def spread(meta, h_rows, c_rows, row0):
    groups = meta.shape[1]
    table = jnp.concatenate([meta[0], meta[1], jnp.zeros((LANES - 2 * groups, LANES), jnp.float32)], axis=0).T
    for g in range(groups):
        at = pl.ds(pl.multiple_of(row0 + g * LANES, LANES), LANES)
        c_rows[at, :] = jnp.broadcast_to(table[:, g:g + 1], (LANES, LANES))
        h_rows[at, :] = jnp.broadcast_to(table[:, groups + g:groups + g + 1], (LANES, LANES))


def append(meta, cols, at, start, size):
    for g in range(size // LANES):
        for m in range(2):
            cols[m:m + 1, pl.ds(pl.multiple_of(at + g * LANES, LANES), LANES)] = meta[m, start // LANES + g:start // LANES + g + 1, :]
    cols[:, pl.ds(pl.multiple_of(at + size, LANES), TILE_J)] = jnp.zeros((2, TILE_J), jnp.float32)


def begin_kernel(scale, pos_ref, q_ref, count_ref, meta, x_row, h_rows, c_rows, x_col, cols, pulls, sums):
    rows, width = pos_ref.shape
    lane = lax.broadcasted_iota(jnp.int32, (LANES, LANES), 1)
    table = jnp.zeros((LANES, LANES), jnp.float32)
    for b in range(rows // LANES):
        x = pos_ref[b * LANES:(b + 1) * LANES, :].astype(jnp.float32)
        table = jnp.where(lane == b, jnp.sum(x * x, axis=1, keepdims=True), table)
        meta[0, b:b + 1, :] = jnp.where(lane[:1] + b * LANES < count_ref[0], q_ref[b:b + 1, :], 0.0)
    meta[1] = table.T[:rows // LANES, :] * scale
    meta[2] = jnp.full(meta.shape[1:], count_ref[0], jnp.int32).astype(jnp.float32)
    sums[...] = jnp.zeros_like(sums)
    pulls[...] = jnp.zeros_like(pulls)
    x_row[:rows, :] = pos_ref[...]
    x_col[:rows, :] = pos_ref[...]
    x_col[rows:rows + TILE_J, :] = jnp.zeros((TILE_J, width), x_col.dtype)
    spread(meta, h_rows, c_rows, 0)
    append(meta, cols, 0, 0, rows)
    cols[:, cols.shape[1] - TILE_J:] = jnp.zeros((2, TILE_J), jnp.float32)


def state_shapes(rows, width, null, dtype):
    tall = 2 * rows + TILE_I
    return [pltpu.VMEM((tall, width), dtype), pltpu.VMEM((tall, LANES), jnp.float32), pltpu.VMEM((tall, LANES), jnp.float32),
            pltpu.VMEM((null, width), dtype), pltpu.VMEM((2, null + TILE_J), jnp.float32), pltpu.VMEM((width + 8, tall), jnp.float32),
            pltpu.VMEM((tall, LANES), jnp.float32)]


def begin(positions, charges, counts, null):
    rows, width = positions.shape
    groups = rows // LANES
    outs = pl.pallas_call(
        functools.partial(begin_kernel, math.log2(math.e) * 0.5 / width),
        out_shape=[jax.ShapeDtypeStruct((3, groups, LANES), jnp.float32)] + state_shapes(rows, width, null, positions.dtype),
        in_specs=[VMEM_SPEC, VMEM_SPEC, pl.BlockSpec(memory_space=pltpu.SMEM)],
        out_specs=[VMEM_SPEC] * 8,
        compiler_params=pltpu.CompilerParams(vmem_limit_bytes=4 << 20),
        cost_estimate=pl.CostEstimate(flops=1 << 30, bytes_accessed=1 << 20, transcendentals=0),
        name='begin',
    )(positions, charges.reshape(groups, LANES), counts)
    return outs[0], list(outs[1:])


def pair_kernel(cfg, *refs):
    rows, width, scale, this = cfg['rows'], cfg['width'], cfg['scale'], cfg['stage']
    refs = list(refs)
    metas = {k: refs.pop(0) for k in cfg['names']}
    loads = [refs.pop(0) for _ in range(cfg['loads'])]
    mate_pos = refs.pop(0) if this == 0 else None
    incoming = refs.pop(0) if this == cfg['turn'] else None
    n_state = 8 if this > cfg['turn'] else 7
    del refs[:n_state]
    x_row, h_rows, c_rows, x_col, cols, pulls, sums = refs[:7]
    turned = refs[7] if this >= cfg['turn'] else None
    refs = refs[8 if this >= cfg['turn'] else 7:]
    n_out = (this == cfg['split']) + 2 * (this == len(cfg['plan']) - 1)
    gram_a, gram_b = refs[n_out:n_out + 2]
    extra = refs[:n_out] + refs[n_out + 2:]

    count = {k: jnp.max(metas[k][2, 0:1, :]).astype(jnp.int32) for k in cfg['names']}
    tiles_own = pl.cdiv(count['own'], TILE_I)
    row_mate = pl.multiple_of(up(count['own'], LANES), LANES)
    tiles_both = pl.cdiv(row_mate + count['mate'], TILE_I)

    end = jnp.int32(0)
    lo = jnp.int32(0)
    for stage, chunks in enumerate(cfg['plan'][:this + 1]):
        for k, (name, start, size) in enumerate(chunks):
            if 0 < stage == this:
                at = pl.multiple_of(end, LANES)
                x_col[pl.ds(at, size), :] = loads[k][...]
                x_col[pl.ds(pl.multiple_of(at + size, LANES), TILE_J), :] = jnp.zeros((TILE_J, width), x_col.dtype)
                append(metas[name], cols, at, start, size)
            end = end + up(jnp.clip(count[name] - start, 0, size), LANES)
        tiles = tiles_own if cfg['modes'][stage] == 'own' else tiles_both
        have = pl.cdiv(end, TILE_J) if cfg['close'][stage] else end // TILE_J
        budget = cfg['budget'][stage]
        hi = have if budget is None else jnp.minimum(have, jnp.maximum(lo, budget // jnp.maximum(tiles, 1)))
        if stage < this:
            lo = hi
        if cfg['close'][stage]:
            end = up(end, TILE_J)
    if this == 0:
        x_row[pl.ds(row_mate, rows), :] = mate_pos[...]
        spread(metas['mate'], h_rows, c_rows, row_mate)
    if incoming is not None:
        table = jnp.zeros((LANES, LANES), jnp.float32)
        sub = lax.broadcasted_iota(jnp.int32, (LANES, LANES), 0)
        for g in range(rows // LANES):
            table = jnp.where(sub == g, incoming[width:width + 1, g * LANES:(g + 1) * LANES], table)
        table = table.T
        lane = lax.broadcasted_iota(jnp.int32, (LANES, LANES), 1)
        for g in range(rows // LANES):
            at = slice(g * LANES, (g + 1) * LANES)
            sums[at, :] += jnp.where(lane == 0, table[:, g:g + 1], 0.0)
            for k in range(width // LANES):
                d = slice(k * LANES, (k + 1) * LANES)
                turned[at, d] = (pulls[d, at] + incoming[d, at]).T

    def aligned(pos):
        return pl.ds(pl.multiple_of(pos[0], TILE_I), TILE_I), pl.ds(pl.multiple_of(pos[1], TILE_J), TILE_J)

    def gram(pos, out):
        row, col = aligned(pos)
        out[...] = lax.dot_general(x_row[row, :], x_col[col, :], (((1,), (1,)), ((), ())), preferred_element_type=jnp.float32)

    def weigh(pos, prod, diag):
        row, col = aligned(pos)
        h_row, c_row = h_rows[row, :], c_rows[row, :]
        parts, total = [], None
        for k in range(TILE_J // LANES):
            at = pl.ds(pl.multiple_of(pos[1] + k * LANES, LANES), LANES)
            arg = jnp.minimum(prod[:, k * LANES:(k + 1) * LANES] * (2.0 * scale) - h_row - cols[1:2, at], 0.0)
            w = jnp.exp2(arg) * c_row * cols[0:1, at]
            if diag:
                off = pos[1] + k * LANES
                off = jnp.where(off < row_mate, off - pos[0], 1 << 20)
                w = jnp.where(lax.broadcasted_iota(jnp.int32, (TILE_I, LANES), 0) - lax.broadcasted_iota(jnp.int32, (TILE_I, LANES), 1) == off, 0.0, w)
            total = w if total is None else total + w
            parts.append(w.astype(jnp.bfloat16))
        sums[row, :] += total
        low = jnp.concatenate(parts, axis=1)
        if turned is None:
            pulls[:width, row] += lax.dot_general(x_col[col, :], low, (((0,), (1,)), ((), ())), preferred_element_type=jnp.float32)
        else:
            turned[row, :] += jnp.dot(low, x_col[col, :], preferred_element_type=jnp.float32)

    def run(units, decode, unroll, diag=False):
        @pl.when(units > 0)
        def _():
            first = decode(0)
            gram(first, gram_a)

            def step(p, pos):
                for k in range(unroll):
                    nxt = decode(jnp.minimum(unroll * p + k + 1, units - 1))
                    gram(nxt, (gram_a, gram_b)[(k + 1) % 2])
                    weigh(pos, (gram_a, gram_b)[k % 2], diag)
                    pos = nxt
                return pos

            def single(unit, pos):
                nxt = decode(jnp.minimum(unit + 1, units - 1))
                weigh(pos, gram_a, diag)
                gram(nxt, gram_a)
                return nxt

            whole = units // unroll
            last = lax.fori_loop(0, whole, step, first)
            if not diag:
                lax.fori_loop(whole * unroll, units, single, last)

    if this == 0:
        per_col = TILE_J // TILE_I
        rest = jnp.maximum(tiles - per_col, per_col * hi - per_col)

        def off_diag(unit):
            j = unit // jnp.maximum(rest, 1)
            i = unit - j * rest
            return jnp.where(i < per_col * j, i, i + per_col) * TILE_I, j * TILE_J

        run(per_col * hi, lambda unit: (unit * TILE_I, unit // per_col * TILE_J), per_col, diag=True)
        run(jnp.where(rest > 0, rest * hi, 0), off_diag, UNROLL)
    elif cfg['loads']:
        def plain(unit):
            j = unit // tiles
            return (unit - j * tiles) * TILE_I, (j + lo) * TILE_J

        run((hi - lo) * tiles, plain, UNROLL)

    if this == cfg['split']:
        lane = lax.broadcasted_iota(jnp.int32, (LANES, LANES), 1)
        table = jnp.zeros((LANES, LANES), jnp.float32)
        for g in range(rows // LANES):
            at = pl.ds(pl.multiple_of(row_mate + g * LANES, LANES), LANES)
            table = jnp.where(lane == g, jnp.sum(sums[at, :], axis=1, keepdims=True), table)
        table = table.T
        extra[0][:width, :] = pulls[:width, pl.ds(row_mate, rows)]
        for g in range(rows // LANES):
            extra[0][width:, g * LANES:(g + 1) * LANES] = jnp.broadcast_to(table[g:g + 1, :], (8, LANES))
    if this == len(cfg['plan']) - 1:
        force, part = extra[:2]
        staged, copy_sem = extra[2:]
        part[...] = jnp.zeros_like(part)
        step = rows // copy_sem.shape[0]

        def tile(i, carry):
            at = pl.ds(pl.multiple_of(i * LANES, LANES), LANES)
            live = lax.broadcasted_iota(jnp.int32, (LANES, LANES), 0) + i * LANES < count['own']
            lanes = jnp.where(live, sums[at, :], 0.0)
            total = jnp.sum(lanes, axis=1, keepdims=True)
            for k in range(width // LANES):
                d = pl.ds(k * LANES, LANES)
                value = total * x_row[at, d].astype(jnp.float32) - turned[at, d]
                staged[at, d] = jnp.where(live, value * cfg['inv_len2'], 0.0)
            part[...] += jnp.sum(lanes.reshape(LANES // 8, 8, LANES), axis=0)
            return carry

        copies = []
        for q in range(copy_sem.shape[0]):
            lax.fori_loop(q * step // LANES, (q + 1) * step // LANES, tile, 0, unroll=True)
            at = pl.ds(q * step, step)
            copies.append(pltpu.make_async_copy(staged.at[at, :], force.at[at, :], copy_sem.at[q]))
            copies[-1].start()
        for copy in copies:
            copy.wait()


def pair_call(cfg, stage, metas, chunks, state, mate_pos=None, incoming=None):
    rows, width = cfg['rows'], cfg['width']
    names = ['own', 'mate']
    for chunk in cfg['plan'][:stage + 1]:
        names += [c[0] for c in chunk if c[0] not in names]
    final = stage == len(cfg['plan']) - 1
    cfg = dict(cfg, stage=stage, names=names, loads=len(chunks) if stage else 0)
    args = [metas[k] for k in names] + (list(chunks) if stage else [mate_pos])
    if incoming is not None:
        args.append(incoming)
    aliases = {}
    for k, a in enumerate(state):
        aliases[len(args)] = k
        args.append(a)
    out_shape = state_shapes(rows, width, cfg['null'], jnp.bfloat16)
    if stage >= cfg['turn']:
        out_shape.append(pltpu.VMEM((rows, width), jnp.float32))
    n_state = len(out_shape)
    if stage == cfg['split']:
        out_shape.append(jax.ShapeDtypeStruct((width + 8, rows), jnp.float32))
    if final:
        out_shape += [jax.ShapeDtypeStruct((rows, width), jnp.float32), jax.ShapeDtypeStruct((8, LANES), jnp.float32)]
    out_specs = [VMEM_SPEC] * len(out_shape)
    scratch = []
    if final:
        out_specs[n_state] = pl.BlockSpec(memory_space=pltpu.HBM)
        scratch = [pltpu.VMEM((rows, width), jnp.float32), pltpu.SemaphoreType.DMA((4,))]
    outs = pl.pallas_call(
        functools.partial(pair_kernel, cfg),
        out_shape=out_shape,
        in_specs=[VMEM_SPEC] * len(args),
        out_specs=out_specs,
        input_output_aliases=aliases,
        scratch_shapes=[pltpu.VMEM((TILE_I, TILE_J), jnp.float32)] * 2 + scratch,
        compiler_params=pltpu.CompilerParams(vmem_limit_bytes=VMEM_MB[stage] << 20),
        cost_estimate=pl.CostEstimate(flops=1 << 30, bytes_accessed=1 << 20, transcendentals=0),
    )(*args)
    return list(outs[:n_state]), outs[n_state:]


def solution(mesh):
    n = mesh.shape['row']
    forth = [(p, (p + 2) % n if p % 2 == 0 else (p - 2) % n) for p in range(n)]
    back = [(b, a) for a, b in forth]
    twice = [(p, (p + n // 2) % n) for p in range(n)]
    swap = [(p, p ^ 1) for p in range(n)]

    def move(x, perm):
        return lax.ppermute(x, 'row', perm)

    def body(positions, charges, counts):
        block_rows, width = positions.shape
        half_rows = block_rows // 2

        def upper(name):
            return name, 0, half_rows

        def lower(name):
            return name, half_rows, block_rows - half_rows

        plan = [[('own', 0, block_rows)], [upper('near'), upper('next')], [lower('near'), lower('next')],
                [upper('far')], [lower('far')], [], [lower('away')]]
        null = up(sum(c[2] for stage in plan for c in stage), TILE_J) + 8 * TILE_J
        cfg = dict(rows=block_rows, width=width, null=null, plan=plan, modes=['both'] * 4 + ['own'] * 3,
                   close=[True, False, False, True, False, False, True],
                   budget=[None, BUDGET] + [None] * 5,
                   split=3, turn=5, scale=math.log2(math.e) * 0.5 / width, inv_len2=1.0 / width)

        mate_pos = move(positions, swap)
        top, bottom = positions[:half_rows], positions[half_rows:]
        meta, state = begin(positions, charges, counts, null)
        near_a, next_a = move(top, forth), move(top, back)
        near_b, next_b = move(bottom, forth), move(bottom, back)
        far_a, far_b = move(near_a, forth), move(near_b, forth)
        away_b = move(far_b, swap)
        far_meta = move(meta, twice)
        metas = {'own': meta, 'mate': move(meta, swap), 'near': move(meta, forth), 'next': move(meta, back),
                 'far': far_meta, 'away': move(far_meta, swap)}
        arrays = [[positions], [near_a, next_a], [near_b, next_b], [far_a], [far_b], [], [away_b]]
        incoming = None
        for stage in range(len(plan)):
            state, out = pair_call(cfg, stage, metas, arrays[stage], state, mate_pos=mate_pos if stage == 0 else None,
                                   incoming=incoming if stage == cfg['turn'] else None)
            if stage == cfg['split']:
                incoming = move(out[0], swap)
        forces, part = out
        return forces, total_energy(part, n)

    row_spec = P(('sys', 'row'), None)
    vec_spec = P(('sys', 'row'))
    step = jax.shard_map(body, mesh=mesh, in_specs=(row_spec, vec_spec, vec_spec), out_specs=(row_spec, P('sys')), check_vma=False)

    def program(positions, charges, counts):
        jax.eval_shape(step, positions, charges, counts)
        return step(positions, charges, counts)

    return program
```
